256 devices in a mesh: leaf: 64 (over y, z, core), grid: 4 (over x).
Axes of the slice: x: 4, y: 4, z: 8, core: 2. Of those that a mesh axis runs over, the one named last changes fastest.
Arguments:
- source_leaf: float32 [8, 32768], P(None, ('leaf', 'grid')), may hold values from -6 to 6
- block_leaf: float32 [32768, 128], P(('leaf', 'grid')), may hold values from -0.5 to 0.5
- expand_leaf: float32 [32768, 128], P(('leaf', 'grid')), may hold values from -0.5 to 0.5
- basis_leaf: float32 [32768, 256], P(('leaf', 'grid')), may hold values from -0.25 to 0.25
- pivot_leaf: float32 [32768], P(('leaf', 'grid')), may hold values from -2 to 2
- couple_leaf: float32 [65536, 128], P(('leaf', 'grid')), may hold values from -0.5 to 0.5
- ranks_leaf: int32 [64, 2], replicated, may hold values from 32 to 128
- targets_leaf: int32 [65536], P(('leaf', 'grid')), may hold values from 0 to 16383, as said below
- source_middle: float32 [8, 32768], P(None, ('leaf', 'grid')), may hold values from -6 to 6
- block_middle: float32 [32768, 128], P(('leaf', 'grid')), may hold values from -0.5 to 0.5
- expand_middle: float32 [32768, 128], P(('leaf', 'grid')), may hold values from -0.5 to 0.5
- basis_middle: float32 [32768, 256], P(('leaf', 'grid')), may hold values from -0.0625 to 0.0625
- pivot_middle: float32 [32768], P(('leaf', 'grid')), may hold values from -2 to 2
- couple_middle: float32 [32768, 128], P(('leaf', 'grid')), may hold values from -0.5 to 0.5
- ranks_middle: int32 [4, 2], replicated, may hold values from 32 to 128
- targets_middle: int32 [32768], P(('leaf', 'grid')), may hold values from 0 to 32767, as said below
- source_upper: float32 [8, 32768], P(None, ('leaf', 'grid')), may hold values from -6 to 6
- block_upper: float32 [32768, 128], P(('leaf', 'grid')), may hold values from -0.5 to 0.5
- expand_upper: float32 [32768, 128], P(('leaf', 'grid')), may hold values from -0.5 to 0.5
- basis_upper: float32 [32768, 256], P(('leaf', 'grid')), may hold values from -0.046875 to 0.046875
- pivot_upper: float32 [32768], P(('leaf', 'grid')), may hold values from -2 to 2
- couple_upper: float32 [32768, 128], P(('leaf', 'grid')), may hold values from -0.5 to 0.5
- ranks_upper: int32 [2, 2], replicated, may hold values from 32 to 128
- targets_upper: int32 [32768], P(('leaf', 'grid')), may hold values from 0 to 32767, as said below
- source_root: float32 [8, 32768], P(None, ('leaf', 'grid')), may hold values from -6 to 6
- block_root: float32 [32768, 128], P(('leaf', 'grid')), may hold values from -0.5 to 0.5
- expand_root: float32 [32768, 128], P(('leaf', 'grid')), may hold values from -0.5 to 0.5
- basis_root: float32 [32768, 256], P(('leaf', 'grid')), may hold values from -0.03125 to 0.03125
- pivot_root: float32 [32768], P(('leaf', 'grid')), may hold values from -2 to 2
- ranks_root: int32 [1, 2], replicated, may hold values from 32 to 128
Outputs:
- answer_leaf: float32 [8, 32768], P(None, ('leaf', 'grid'))
- answer_middle: float32 [8, 32768], P(None, ('leaf', 'grid'))
- answer_upper: float32 [8, 32768], P(None, ('leaf', 'grid'))
- answer_root: float32 [8, 32768], P(None, ('leaf', 'grid'))
The draws below stay inside these ranges and needn't reach their ends.
Inputs may be any that keep to these rules, and one draw needn't show every extreme that they name: `targets_leaf`: within one leaf front the 1024 entries are distinct; each names a row of the parent front's row vector of 16384 rows. Split that vector's separator part and its update part each evenly, in order, over the parent's devices (leaf then grid); then the rows of one device name at most 4 rows held by any one of them, and exactly that many for some. `targets_middle`: within one middle front the entries are distinct; each names a row of the parent front's row vector of 32768 rows. Split likewise over the parent's devices, the rows of one device name at most 1 row held by any one of them, and exactly that many for some. `targets_upper`: within one upper front the entries are distinct; each names a row of the root separator. Split evenly in order over all devices, the rows of one device name at most 1 row held by any one of them, and exactly that many for some.
All inputs are finite; a program needn't handle non-finite values.
Results may differ from the reference program's by a relative error of at most 0.0003.
Values sent between devices are 32-bit elements; how exact they have to be, the bound alone decides.
A program may use at most 128 MiB of HBM per device.

```python
import jax
import jax.numpy as jnp
from jax import lax

RHS_COUNT = 8
BLOCK = 128
RANK = 128
TOP_ROWS = 128
SEP_LEAF = 512
UPD_LEAF = 1024
SEP_MID = 8192
SEP_UP = 16384
SEP_ROOT = 32768
N_LEAF = 64
N_GRID = 4


def pick_rows(key, salt, fronts, count, owners, width, pieces, sep_rows):
    base = jax.random.fold_in(key, salt)
    slots_each = pieces * width

    def one_front(front):
        fkey = jax.random.fold_in(base, front)
        order = jax.random.permutation(jax.random.fold_in(fkey, 1), owners)
        slot_keys = jax.vmap(lambda owner: jax.random.fold_in(jax.random.fold_in(fkey, 2), owner))(jnp.arange(owners, dtype=jnp.int32))
        slot_order = jax.vmap(lambda one: jax.random.permutation(one, slots_each))(slot_keys)
        rows = jnp.arange(count, dtype=jnp.int32)
        owner = order[rows % owners]
        slot = slot_order[owner, rows // owners]
        return slot // width * sep_rows + owner * width + slot % width
    picked = jax.vmap(one_front)(jnp.arange(fronts, dtype=jnp.int32))
    return picked.reshape(-1).astype(jnp.int32)


def draw_targets_leaf(key, part):
    return pick_rows(key, 11, N_LEAF, UPD_LEAF, N_LEAF * N_GRID // 4, TOP_ROWS, 2, SEP_MID)


def draw_targets_middle(key, part):
    return pick_rows(key, 12, 4, SEP_MID, N_LEAF * N_GRID // 2, TOP_ROWS, 2, SEP_UP)


def draw_targets_upper(key, part):
    return pick_rows(key, 13, 2, SEP_UP, N_LEAF * N_GRID, TOP_ROWS, 1, SEP_ROOT)


def set_ends(array, own_key, low, top_value):
    longest = array.shape.index(max(array.shape))
    spots = []
    for shift in (0, 1):
        where = [jax.random.randint(jax.random.fold_in(own_key, axis), (), 0, length) for axis, length in enumerate(array.shape)]
        where[longest] = (where[longest] + shift) % array.shape[longest]
        spots.append(tuple(where))
    return array.at[spots[0]].set(low).at[spots[1]].set(top_value)


def level_of(rng, dims, shards, least, high):
    def one(position, blocks):
        heights = jax.random.uniform(jax.random.fold_in(jax.random.fold_in(rng, 6), position), (blocks,), jnp.float32, least / len(shards), high / len(shards))
        return jnp.repeat(jnp.exp(heights), dims[position] // blocks).reshape((-1,) + (1,) * (len(dims) - position - 1))

    factor_of = one(*shards[0])
    for cut in shards[1:]:
        factor_of = factor_of * one(*cut)
    return factor_of


def centred(key, dims, scale, limit, shards=(), held_as=jnp.bfloat16):
    factor_of = level_of(key, dims, shards, -0.22, 0.18) if shards else 1.0
    values = jax.random.normal(key, dims, jnp.float32) * scale * factor_of
    return jnp.minimum(jnp.maximum(values, -limit), limit).astype(held_as)


def setup_inputs(seed: int = 0) -> dict:
    key_list = jax.random.split(jax.random.key(seed), 31)
    return {
        "source_leaf": centred(key_list[0], (RHS_COUNT, N_LEAF * SEP_LEAF), 1.0, 6.0, ((1, 256),), jnp.float32),
        "block_leaf": centred(key_list[1], (N_LEAF * SEP_LEAF, BLOCK), BLOCK ** -0.5, 0.5, ((0, 256),), jnp.float32),
        "expand_leaf": centred(key_list[2], (N_LEAF * SEP_LEAF, RANK), RANK ** -0.5, 0.5, ((0, 256),), jnp.float32),
        "basis_leaf": centred(key_list[3], (N_LEAF * SEP_LEAF, 2 * RANK), SEP_LEAF ** -0.5, 0.25, ((0, 256),), jnp.float32),
        "pivot_leaf": jnp.clip(jax.random.uniform(key_list[4], (N_LEAF * SEP_LEAF,), jnp.float32, -2.0, 2.0) * level_of(key_list[4], (N_LEAF * SEP_LEAF,), ((0, 256),), -0.4, 0.0), -2.0, 2.0),
        "couple_leaf": centred(key_list[5], (N_LEAF * UPD_LEAF, RANK), RANK ** -0.5, 0.5, ((0, 256),), jnp.float32),
        "ranks_leaf": set_ends(jax.random.randint(key_list[6], (N_LEAF, 2), RANK // 4, RANK + 1), jax.random.fold_in(key_list[6], 1), RANK // 4, RANK).astype(jnp.int32),
        "targets_leaf": draw_targets_leaf(jax.random.fold_in(key_list[30], 71), 0),
        "source_middle": centred(key_list[8], (RHS_COUNT, 4 * SEP_MID), 1.0, 6.0, ((1, 256),), jnp.float32),
        "block_middle": centred(key_list[9], (4 * SEP_MID, BLOCK), BLOCK ** -0.5, 0.5, ((0, 256),), jnp.float32),
        "expand_middle": centred(key_list[10], (4 * SEP_MID, RANK), RANK ** -0.5, 0.5, ((0, 256),), jnp.float32),
        "basis_middle": centred(key_list[11], (4 * SEP_MID, 2 * RANK), SEP_MID ** -0.5, 0.0625, ((0, 256),), jnp.float32),
        "pivot_middle": jnp.clip(jax.random.uniform(key_list[12], (4 * SEP_MID,), jnp.float32, -2.0, 2.0) * level_of(key_list[12], (4 * SEP_MID,), ((0, 256),), -0.4, 0.0), -2.0, 2.0),
        "couple_middle": centred(key_list[13], (4 * SEP_MID, RANK), RANK ** -0.5, 0.5, ((0, 256),), jnp.float32),
        "ranks_middle": set_ends(jax.random.randint(key_list[14], (4, 2), RANK // 4, RANK + 1), jax.random.fold_in(key_list[14], 1), RANK // 4, RANK).astype(jnp.int32),
        "targets_middle": draw_targets_middle(jax.random.fold_in(key_list[30], 71), 0),
        "source_upper": centred(key_list[16], (RHS_COUNT, 2 * SEP_UP), 1.0, 6.0, ((1, 256),), jnp.float32),
        "block_upper": centred(key_list[17], (2 * SEP_UP, BLOCK), BLOCK ** -0.5, 0.5, ((0, 256),), jnp.float32),
        "expand_upper": centred(key_list[18], (2 * SEP_UP, RANK), RANK ** -0.5, 0.5, ((0, 256),), jnp.float32),
        "basis_upper": centred(key_list[19], (2 * SEP_UP, 2 * RANK), SEP_UP ** -0.5, 0.046875, ((0, 256),), jnp.float32),
        "pivot_upper": jnp.clip(jax.random.uniform(key_list[20], (2 * SEP_UP,), jnp.float32, -2.0, 2.0) * level_of(key_list[20], (2 * SEP_UP,), ((0, 256),), -0.4, 0.0), -2.0, 2.0),
        "couple_upper": centred(key_list[21], (2 * SEP_UP, RANK), RANK ** -0.5, 0.5, ((0, 256),), jnp.float32),
        "ranks_upper": set_ends(jax.random.randint(key_list[22], (2, 2), RANK // 4, RANK + 1), jax.random.fold_in(key_list[22], 1), RANK // 4, RANK).astype(jnp.int32),
        "targets_upper": draw_targets_upper(jax.random.fold_in(key_list[30], 71), 0),
        "source_root": centred(key_list[24], (RHS_COUNT, SEP_ROOT), 1.0, 6.0, ((1, 256),), jnp.float32),
        "block_root": centred(key_list[25], (SEP_ROOT, BLOCK), BLOCK ** -0.5, 0.5, ((0, 256),), jnp.float32),
        "expand_root": centred(key_list[26], (SEP_ROOT, RANK), RANK ** -0.5, 0.5, ((0, 256),), jnp.float32),
        "basis_root": centred(key_list[27], (SEP_ROOT, 2 * RANK), SEP_ROOT ** -0.5, 0.03125, ((0, 256),), jnp.float32),
        "pivot_root": jnp.clip(jax.random.uniform(key_list[28], (SEP_ROOT,), jnp.float32, -2.0, 2.0) * level_of(key_list[28], (SEP_ROOT,), ((0, 256),), -0.4, 0.0), -2.0, 2.0),
        "ranks_root": jax.random.randint(key_list[29], (1, 2), RANK // 4, RANK + 1).astype(jnp.int32),
    }


HIGH_PRECISION = lax.Precision.HIGHEST


def make_masks(ranks):
    cols = jnp.arange(RANK, dtype=jnp.int32)
    head_mask_grid = (cols[None, :] < ranks[:, 0:1]).astype(jnp.float32)[:, None, :]
    column_mask_grid = (cols[None, :] < ranks[:, 1:2]).astype(jnp.float32)[:, None, :]
    return head_mask_grid, column_mask_grid


def forward(source, inc_sep, block, expand, basis, pivot, ranks, fronts):
    width = source.shape[1] // fronts
    level_batch_index = source.reshape(RHS_COUNT, fronts, width).transpose(1, 0, 2)
    if inc_sep is not None:
        level_batch_index = level_batch_index + inc_sep
    tiles = block.reshape(fronts, width // BLOCK, BLOCK, BLOCK)
    local_portion = jnp.einsum("fanh,fnhk->fank", level_batch_index.reshape(fronts, RHS_COUNT, width // BLOCK, BLOCK), tiles, precision=HIGH_PRECISION).reshape(fronts, RHS_COUNT, width)
    gens = basis.reshape(fronts, width, 2 * RANK)
    query_lookup = gens[:, :, :RANK]
    coupling_right_factor = gens[:, :, RANK:]
    spread_across_rows = expand.reshape(fronts, width, RANK)
    head_mask_grid, column_mask_grid = make_masks(ranks)
    hidden_query_rows = jnp.einsum("mle,meq->mlq", level_batch_index, query_lookup, precision=HIGH_PRECISION) * head_mask_grid
    intermediate_entries = local_portion + jnp.einsum("gdk,gtk->gdt", hidden_query_rows, spread_across_rows, precision=HIGH_PRECISION)
    weight_entries = jnp.einsum("mle,meq->mlq", intermediate_entries, coupling_right_factor, precision=HIGH_PRECISION) * column_mask_grid
    correction_entries = intermediate_entries * pivot.reshape(fronts, 1, width)
    return correction_entries, weight_entries, (tiles, query_lookup, coupling_right_factor, spread_across_rows, head_mask_grid, column_mask_grid)


def flat_index(targets, fronts, parents, total):
    count = targets.shape[0] // fronts
    owner = jnp.arange(fronts, dtype=jnp.int32) // (fronts // parents)
    return (owner[:, None] * total + targets.reshape(fronts, count).astype(jnp.int32)).reshape(-1)


def scatter_up(update, targets, fronts, parents, sep_par, upd_par):
    total = sep_par + upd_par
    flat = flat_index(targets, fronts, parents, total)
    values = update.transpose(1, 0, 2).reshape(RHS_COUNT, -1)
    buffer = jnp.zeros((RHS_COUNT, parents * total), jnp.float32).at[:, flat].add(values)
    buffer = buffer.reshape(RHS_COUNT, parents, total).transpose(1, 0, 2)
    return buffer[:, :, :sep_par], buffer[:, :, sep_par:]


def pull_down(front_rows, targets, fronts, parents):
    total = front_rows.shape[2]
    flat = flat_index(targets, fronts, parents, total)
    whole = front_rows.transpose(1, 0, 2).reshape(RHS_COUNT, parents * total)
    values = jnp.take(whole, flat, axis=1)
    return values.reshape(RHS_COUNT, fronts, -1).transpose(1, 0, 2)


def backward(correction_entries, x_upd, couple, parts, fronts):
    tiles, query_lookup, coupling_right_factor, spread_across_rows, head_mask_grid, column_mask_grid = parts
    width = correction_entries.shape[2]
    remainder_rows = correction_entries
    if x_upd is not None:
        couple_u = couple.reshape(fronts, -1, RANK)
        solve_direction = jnp.einsum("fau,fur->far", x_upd, couple_u, precision=HIGH_PRECISION) * column_mask_grid
        remainder_rows = correction_entries - jnp.einsum("gdk,gtk->gdt", solve_direction, coupling_right_factor, precision=HIGH_PRECISION)
    right_projection = jnp.einsum("mle,meq->mlq", remainder_rows, spread_across_rows, precision=HIGH_PRECISION) * head_mask_grid
    local_portion = jnp.einsum("fanh,fnkh->fank", remainder_rows.reshape(fronts, RHS_COUNT, width // BLOCK, BLOCK), tiles, precision=HIGH_PRECISION).reshape(fronts, RHS_COUNT, width)
    return local_portion + jnp.einsum("gdk,gtk->gdt", right_projection, query_lookup, precision=HIGH_PRECISION)


def reference(source_leaf, block_leaf, expand_leaf, basis_leaf, pivot_leaf, couple_leaf, ranks_leaf, targets_leaf,
              source_middle, block_middle, expand_middle, basis_middle, pivot_middle, couple_middle, ranks_middle, targets_middle,
              source_upper, block_upper, expand_upper, basis_upper, pivot_upper, couple_upper, ranks_upper, targets_upper,
              source_root, block_root, expand_root, basis_root, pivot_root, ranks_root):
    levels = [
        (source_leaf, block_leaf, expand_leaf, basis_leaf, pivot_leaf, couple_leaf, ranks_leaf, targets_leaf),
        (source_middle, block_middle, expand_middle, basis_middle, pivot_middle, couple_middle, ranks_middle, targets_middle),
        (source_upper, block_upper, expand_upper, basis_upper, pivot_upper, couple_upper, ranks_upper, targets_upper),
        (source_root, block_root, expand_root, basis_root, pivot_root, None, ranks_root, None),
    ]
    fronts = [N_LEAF, 4, 2, 1]
    inc_sep = None
    inc_upd = None
    saved = []
    for level in range(4):
        source, block, expand, basis, pivot, couple, ranks, targets = levels[level]
        correction_entries, weight_entries, parts = forward(source, inc_sep, block, expand, basis, pivot, ranks, fronts[level])
        saved.append((correction_entries, parts))
        if level < 3:
            couple_u = couple.reshape(fronts[level], -1, RANK)
            update = -jnp.einsum("far,fur->fau", weight_entries, couple_u, precision=HIGH_PRECISION)
            if inc_upd is not None:
                update = update + inc_upd
            sep_par = levels[level + 1][0].shape[1] // fronts[level + 1]
            upd_par = 0
            if level + 1 < 3:
                upd_par = levels[level + 1][5].shape[0] // fronts[level + 1]
            inc_sep, inc_upd = scatter_up(update, targets, fronts[level], fronts[level + 1], sep_par, upd_par)
            if upd_par == 0:
                inc_upd = None
    answers = [None, None, None, None]
    rows_par = None
    for level in (3, 2, 1, 0):
        correction_entries, parts = saved[level]
        couple = levels[level][5]
        targets = levels[level][7]
        x_upd = None
        if level < 3:
            x_upd = pull_down(rows_par, targets, fronts[level], fronts[level + 1])
        xvals = backward(correction_entries, x_upd, couple, parts, fronts[level])
        answers[level] = xvals.transpose(1, 0, 2).reshape(RHS_COUNT, -1)
        rows_par = xvals if x_upd is None else jnp.concatenate([xvals, x_upd], axis=2)
    return (answers[0], answers[1], answers[2], answers[3])
```

```python
import functools

import jax
import jax.numpy as jnp
from jax import lax
from jax.experimental import pallas as pl
from jax.experimental.pallas import tpu as pltpu
from jax.sharding import PartitionSpec as P

MESH = pl.DeviceIdType.MESH
HIGHEST = lax.Precision.HIGHEST

NX, NZC, NY = 4, 16, 4

EXCHANGES = [
    ("x0", 4, 144),
    ("zp0", 4, 8),
    ("w0", 16, 8),
    ("a1", 16, 24),
    ("a2", 4, 80),
    ("b1", 16, 16),
    ("b2", 8, 32),
    ("c1", 16, 24),
    ("c2", 16, 32),
    ("cr_xc", 8, 48),
    ("cr_z", 8, 48),
    ("cr_m", 8, 16),
    ("cr_y", 4, 32),
    ("cr_g", 8, 48),
    ("f1_xc", 8, 16),
    ("f1_z", 8, 16),
    ("f1_y", 2, 8),
    ("f2_xc", 8, 24),
    ("f2_z", 8, 24),
    ("f2_y", 4, 24),
    ("f3_xc", 8, 24),
    ("f3_z", 8, 24),
    ("f3_y", 4, 24),
    ("d1", 16, 8),
    ("d2", 8, 16),
    ("e1", 16, 16),
    ("e2", 16, 16),
    ("u2_xc", 8, 16),
    ("u2_z", 8, 16),
    ("u2_y", 4, 16),
    ("g1", 16, 16),
    ("g2", 16, 16),
    ("u1_xc", 8, 16),
    ("u1_z", 8, 16),
    ("u1_y", 2, 16),
    ("h1", 8, 16),
    ("h2", 16, 8),
    ("u0_zc", 16, 8),
    ("u0_x", 4, 8),
]
NAMES = [entry[0] for entry in EXCHANGES]
SCATTERED = ["a1", "a2", "b1", "b2", "c1", "c2", "cr_xc", "d1", "d2", "e1", "e2", "g1", "g2", "h1", "h2", "u0_zc"]


def dot(a, b, ca, cb):
    return lax.dot_general(
        a, b, (((ca,), (cb,)), ((), ())), precision=HIGHEST, preferred_element_type=jnp.float32
    )


def mm(a, b):
    return dot(a, b, 1, 0)


def mm_t(a, b):
    return dot(a, b, 1, 1)


def t_mm(a, b):
    return dot(a, b, 0, 0)


def iota(shape, dim):
    return lax.broadcasted_iota(jnp.int32, shape, dim)


def ones_where(cond):
    return jnp.where(cond, 1.0, 0.0).astype(jnp.float32)


def stack16(v):
    return jnp.concatenate([v] * 16, axis=0)


def kernel(*refs):
    (
        src0, blk0, exp0, bas0, piv0, cpl0, rnk0, tgt0,
        src1, blk1, exp1, bas1, piv1, cpl1, rnk1, tgt1,
        src2, blk2, exp2, bas2, piv2, cpl2, rnk2, tgt2,
        src3, blk3, exp3, bas3, piv3, rnk3,
        out0, out1, out2, out3,
    ) = refs[:34]
    n_ex = len(EXCHANGES)
    recv = dict(zip(NAMES, refs[34 : 34 + n_ex]))
    send = dict(zip(SCATTERED, refs[34 + n_ex : 34 + n_ex + len(SCATTERED)]))
    send_sem, recv_sem = refs[34 + n_ex + len(SCATTERED) :]

    leaf = lax.axis_index("leaf")
    x = lax.axis_index("grid")
    y = leaf // 16
    zc = leaf % 16
    z = zc // 2
    c = zc % 2
    u = y // 2
    yb = y % 2
    xc = x * 2 + c
    k8 = yb * 4 + x
    k16 = y * 4 + x

    axes = {
        "x": (x, 4, lambda d: (leaf, d)),
        "zc": (zc, 16, lambda d: (y * 16 + d, x)),
        "xc": (xc, 8, lambda d: (leaf - c + d % 2, d // 2)),
        "z": (z, 8, lambda d: (y * 16 + d * 2 + c, x)),
        "y2": (yb, 2, lambda d: ((u * 2 + d) * 16 + zc, x)),
        "y4": (y, 4, lambda d: (d * 16 + zc, x)),
        "k8": (k8, 8, lambda d: ((u * 2 + d // 4) * 16 + zc, d % 4)),
        "k16": (k16, 16, lambda d: ((d // 4) * 16 + zc, d % 4)),
    }
    pending = []

    def copy_of(name, src, dst, dev):
        i = NAMES.index(name)
        return pltpu.make_async_remote_copy(
            src_ref=src,
            dst_ref=dst,
            send_sem=send_sem.at[i],
            recv_sem=recv_sem.at[i],
            device_id=dev,
            device_id_type=MESH,
        )

    def start(name, axis):
        me, n, dev = axes[axis]
        buf = recv[name]
        scattered = name in send

        def body(o, carry):
            d = lax.rem(me + o, n)
            src = send[name].at[d] if scattered else buf.at[me]
            copy_of(name, src, buf.at[me], dev(d)).start()
            return carry

        if scattered:
            buf[me] = send[name][me]
        lax.fori_loop(1, n, body, 0)
        pending.append((name, axis))

    def whole(name, axis):
        me, n, dev = axes[axis]
        part = recv[name].at[pl.ds(0, n - 1)]
        return copy_of(name, part, part, dev(lax.rem(me + 1, n)))

    def wait(name, axis):
        whole(name, axis).wait_recv()

    def share(name, axis, value):
        recv[name][axes[axis][0]] = value
        start(name, axis)

    def total(name, axis):
        wait(name, axis)
        return jnp.sum(recv[name][...], axis=0)

    barrier = pltpu.get_barrier_semaphore()

    def greet(axis):
        me, n, dev = axes[axis]

        def body(o, carry):
            pl.semaphore_signal(barrier, inc=1, device_id=dev(lax.rem(me + o, n)), device_id_type=MESH)
            return carry

        lax.fori_loop(1, n, body, 0)
        return n - 1

    greeted = greet("zc") + greet("k16") + greet("xc")

    lane = iota((1, 128), 1)

    def mask_of(ref, front, side):
        return ones_where(lane < ref[front, side])

    def column(row):
        n = row.shape[1]
        return jnp.transpose(jnp.broadcast_to(row, (128, n)))

    def packets(targets, sep_bits, kbits, ranked):
        piece = targets >> sep_bits
        within = targets & ((1 << sep_bits) - 1)
        label = piece * 128 + (within & 127) + 1
        owner = within >> 7
        if ranked:
            n = targets.shape[1]
            of = owner.astype(jnp.float32)
            same = column(of)[:, 0:1] == of
            before = iota((n, n), 0) < iota((n, n), 1)
            order = jnp.sum(ones_where(same & before), axis=0, keepdims=True)
            return of * 4.0 + order, label.astype(jnp.float32)
        sub = owner & 63
        pos = ((sub >> 2) << kbits) + ((owner >> 6) << 2) + (sub & 3)
        return pos.astype(jnp.float32), label.astype(jnp.float32)

    def place(pos, count):
        n = pos.shape[1]
        return ones_where(iota((count, n), 0).astype(jnp.float32) == pos)

    def label_rows(pos, label, kbits):
        n = pos.shape[1]
        ipos = pos.astype(jnp.int32)
        major = (ipos >> kbits).astype(jnp.float32)
        minor = (ipos & ((1 << kbits) - 1)).astype(jnp.float32)
        pick = ones_where(iota((16, n), 0).astype(jnp.float32) == major)
        spread = jnp.where(iota((n, 128), 1).astype(jnp.float32) == column(minor), column(label), 0.0)
        return mm(pick, spread)

    def fill_packets(name, pos, label, rows, kbits, couple):
        k = 1 << kbits
        at = place(pos, 16 * k)
        send[name][:, 0:k, :] = mm(at, couple).reshape(16, k, 128)
        lab = label_rows(pos, label, kbits)
        send[name][:, k : k + 8, :] = jnp.broadcast_to(lab[:, None, :], (16, 8, 128))
        return at

    pos0, lab0 = packets(tgt0[...], 13, 4, True)
    fill_packets("a1", pos0, lab0, 24, 4, cpl0[...])
    Q0, V0 = bas0[:, 0:128], bas0[:, 128:256]
    loc0 = mm(src0[...], blk0[...])
    x0_own = jnp.concatenate(
        [mm(src0[...], Q0), mm(loc0, V0), t_mm(exp0[...], V0)], axis=0
    )

    pl.semaphore_wait(barrier, greeted)
    share("x0", "x", x0_own)
    start("a1", "zc")

    V1 = bas1[:, 128:256]
    V2 = bas2[:, 128:256]
    cr1_own = t_mm(exp1[...], V1)
    cr2_own = t_mm(exp2[...], V2)
    P3 = exp3[...]
    scaled3 = P3 * column(piv3[...])
    m3_own = t_mm(P3, scaled3)
    send["cr_xc"][:, 0:16, :] = cr1_own.reshape(8, 16, 128)
    send["cr_xc"][:, 16:32, :] = cr2_own.reshape(8, 16, 128)
    send["cr_xc"][:, 32:48, :] = m3_own.reshape(8, 16, 128)
    start("cr_xc", "xc")

    mh0, mc0 = mask_of(rnk0, leaf, 0), mask_of(rnk0, leaf, 1)
    tot0 = total("x0", "x")
    hq0 = tot0[0:8] * mh0
    cr0 = tot0[16:144]
    w0 = (tot0[8:16] + mm(hq0, cr0)) * mc0
    share("w0", "zc", w0)
    z0 = (loc0 + mm_t(hq0, exp0[...])) * piv0[...]
    share("zp0", "x", mm(z0, exp0[...]))

    wait("a1", "zc")
    s_row = iota((256, 256), 0)
    r_col = iota((256, 256), 1)
    turn_a = ones_where(r_col == ((s_row >> 2) & 15) * 16 + (s_row >> 6) * 4 + (s_row & 3))
    moved = mm(turn_a, recv["a1"][:, 0:16, :].reshape(256, 128))
    labels = jnp.max(recv["a1"][:, 16:24, :], axis=1)
    send["a2"][:, 0:64, :] = moved.reshape(4, 64, 128)
    send["a2"][:, 64:80, :] = jnp.broadcast_to(labels[None], (4, 16, 128))
    start("a2", "x")

    cr_z_own = total("cr_xc", "xc")
    share("cr_z", "z", cr_z_own)

    pos1, lab1 = packets(tgt1[...], 14, 3, False)
    at1 = fill_packets("b1", pos1, lab1, 16, 3, cpl1[...])
    start("b1", "zc")
    pos2, lab2 = packets(tgt2[...], 15, 4, False)
    at2 = fill_packets("c1", pos2, lab2, 24, 4, cpl2[...])
    start("c1", "zc")

    wait("w0", "zc")
    wait("a2", "x")
    c0h = recv["a2"][:, 0:64, :].reshape(256, 128)
    lab_in = recv["a2"][:, 64:80, :].reshape(64, 128)
    spread = mm(ones_where(iota((256, 64), 1) == (iota((256, 64), 0) >> 2)), lab_in)
    mine = iota((256, 128), 1) == x * 4 + (iota((256, 128), 0) & 3)
    lab_col = jnp.sum(jnp.where(mine, spread, 0.0), axis=1, keepdims=True)
    oh0 = ones_where(iota((256, 256), 1).astype(jnp.float32) == lab_col - 1.0)
    front0 = (iota((128, 256), 0) >> 3) == ((iota((128, 256), 1) & 63) >> 2)
    e0 = jnp.where(front0, mm_t(recv["w0"][...].reshape(128, 128), c0h), 0.0)
    inc0 = -mm(jnp.sum(e0.reshape(16, 8, 256), axis=0), oh0)
    b1 = src1[...] + inc0[:, 0:128]
    upd1 = inc0[:, 128:256]
    loc1 = mm(b1, blk1[...])
    Q1 = bas1[:, 0:128]
    share("f1_xc", "xc", jnp.concatenate([mm(b1, Q1), mm(loc1, V1)], axis=0))
    send["d1"][...] = mm_t(at1, stack16(upd1)).reshape(16, 8, 128)
    start("d1", "zc")

    cr_sum = total("cr_z", "z")
    share("cr_m", "xc", cr_sum[0:16])
    share("cr_y", "y4", cr_sum[16:48])

    share("f1_z", "z", total("f1_xc", "xc"))

    wait("b1", "zc")
    turn_b = ones_where(iota((128, 128), 1) == (iota((128, 128), 0) & 15) * 8 + (iota((128, 128), 0) >> 4))
    send["b2"][:, 0:16, :] = mm(turn_b, recv["b1"][:, 0:8, :].reshape(128, 128)).reshape(8, 16, 128)
    send["b2"][:, 16:32, :] = jnp.broadcast_to(jnp.max(recv["b1"][:, 8:16, :], axis=1)[None], (8, 16, 128))
    start("b2", "k8")
    wait("d1", "zc")
    send["d2"][...] = mm(turn_b, recv["d1"][...].reshape(128, 128)).reshape(8, 16, 128)
    start("d2", "k8")
    wait("cr_y", "y4")
    cy = recv["cr_y"]
    share(
        "cr_g",
        "xc",
        jnp.concatenate(
            [
                cy[0, 0:16, :] + cy[1, 0:16, :],
                cy[2, 0:16, :] + cy[3, 0:16, :],
                (cy[0, 16:32, :] + cy[1, 16:32, :]) + (cy[2, 16:32, :] + cy[3, 16:32, :]),
            ],
            axis=0,
        ),
    )
    wait("c1", "zc")
    turn_c = ones_where(r_col == (s_row & 15) * 16 + (s_row >> 4))
    send["c2"][:, 0:16, :] = mm(turn_c, recv["c1"][:, 0:16, :].reshape(256, 128)).reshape(16, 16, 128)
    send["c2"][:, 16:32, :] = jnp.broadcast_to(jnp.max(recv["c1"][:, 16:24, :], axis=1)[None], (16, 16, 128))
    start("c2", "k16")

    wait("cr_m", "xc")
    cr1 = recv["cr_m"][...].reshape(128, 128)
    mh1, mc1 = mask_of(rnk1, y, 0), mask_of(rnk1, y, 1)
    tot1 = total("f1_z", "z")
    hq1 = tot1[0:8] * mh1
    share("f1_y", "y2", (tot1[8:16] + mm(hq1, cr1)) * mc1)
    z1 = (loc1 + mm_t(hq1, exp1[...])) * piv1[...]
    zp1_own = mm(z1, exp1[...])

    wait("b2", "k8")
    c1h = recv["b2"][:, 0:16, :].reshape(128, 128)
    lab_in = recv["b2"][:, 16:32, :].reshape(128, 128)
    lab_col = jnp.sum(jnp.where(iota((128, 128), 1) == k8, lab_in, 0.0), axis=1, keepdims=True)
    oh1 = ones_where(iota((128, 256), 1).astype(jnp.float32) == lab_col - 1.0)
    front1 = (iota((16, 128), 0) >> 3) == (iota((16, 128), 1) >> 6)
    wait("d2", "k8")
    came1 = jnp.transpose(recv["d2"][...].reshape(128, 128))[0:8]
    wait("f1_y", "y2")
    e1 = jnp.where(front1, mm_t(recv["f1_y"][...].reshape(16, 128), c1h), 0.0)
    inc1 = mm(came1 - (e1[0:8] + e1[8:16]), oh1)
    b2 = src2[...] + inc1[:, 0:128]
    upd2 = inc1[:, 128:256]
    loc2 = mm(b2, blk2[...])
    Q2 = bas2[:, 0:128]
    share("f2_xc", "xc", jnp.concatenate([mm(b2, Q2), mm(loc2, V2), zp1_own], axis=0))
    send["e1"][...] = mm_t(at2, stack16(upd2)).reshape(16, 16, 128)
    start("e1", "zc")
    share("f2_z", "z", total("f2_xc", "xc"))
    wait("e1", "zc")
    send["e2"][...] = mm(turn_c, recv["e1"][...].reshape(256, 128)).reshape(16, 16, 128)
    start("e2", "k16")
    wait("cr_g", "xc")
    cg = recv["cr_g"]
    cr2_each = [cg[:, 0:16, :].reshape(128, 128), cg[:, 16:32, :].reshape(128, 128)]
    m3 = cg[:, 32:48, :].reshape(128, 128)
    wait("c2", "k16")
    c2h = recv["c2"][:, 0:16, :].reshape(256, 128)
    lab_in = recv["c2"][:, 16:32, :].reshape(256, 128)
    lab_col = jnp.sum(jnp.where(iota((256, 128), 1) == k16, lab_in, 0.0), axis=1, keepdims=True)
    oh2 = ones_where(iota((256, 128), 1).astype(jnp.float32) == lab_col - 1.0)
    front2 = (iota((16, 256), 0) >> 3) == (iota((16, 256), 1) >> 7)
    share("f2_y", "y4", total("f2_z", "z"))
    wait("f2_y", "y4")
    fy = recv["f2_y"]
    hq2_each, w2_each = [], []
    for v in range(2):
        t1 = fy[2 * v, 0:8, :] + fy[2 * v + 1, 0:8, :]
        t2 = fy[2 * v, 8:16, :] + fy[2 * v + 1, 8:16, :]
        hq = t1 * mask_of(rnk2, v, 0)
        hq2_each.append(hq)
        w2_each.append((t2 + mm(hq, cr2_each[v])) * mask_of(rnk2, v, 1))
    zp1 = fy[y, 16:24, :]
    first = u == 0
    hq2 = jnp.where(first, hq2_each[0], hq2_each[1])
    cr2 = jnp.where(first, cr2_each[0], cr2_each[1])
    mh2, mc2 = mask_of(rnk2, u, 0), mask_of(rnk2, u, 1)
    z2 = (loc2 + mm_t(hq2, exp2[...])) * piv2[...]
    zp2_own = mm(z2, exp2[...])

    e2 = jnp.where(front2, mm_t(jnp.concatenate(w2_each, axis=0), c2h), 0.0)
    wait("e2", "k16")
    came2 = jnp.transpose(recv["e2"][...].reshape(256, 128))[0:8]
    b3 = src3[...] + mm(came2 - (e2[0:8] + e2[8:16]), oh2)
    loc3 = mm(b3, blk3[...])
    Q3 = bas3[:, 0:128]
    share("f3_xc", "xc", jnp.concatenate([mm(b3, Q3), mm(loc3 * piv3[...], P3), zp2_own], axis=0))
    share("f3_z", "z", total("f3_xc", "xc"))
    share("f3_y", "y4", total("f3_z", "z"))
    wait("f3_y", "y4")
    fy = recv["f3_y"]
    lower = fy[0] + fy[1]
    upper = fy[2] + fy[3]
    mh3 = mask_of(rnk3, 0, 0)
    both = lower + upper
    hq3 = both[0:8] * mh3
    zp2 = jnp.where(first, lower[16:24], upper[16:24])
    g3 = (both[8:16] + mm(hq3, m3)) * mh3
    z3 = (loc3 + mm_t(hq3, P3)) * piv3[...]
    x3 = mm_t(z3, blk3[...]) + mm_t(g3, Q3)
    out3[...] = x3

    vals = mm_t(x3, oh2)
    share("u2_xc", "xc", mm(jnp.where(front2, jnp.concatenate([vals, vals], axis=0), 0.0), c2h))
    send["g1"][...] = mm_t(oh2, stack16(x3)).reshape(16, 16, 128)
    start("g1", "k16")
    share("u2_z", "z", total("u2_xc", "xc"))
    wait("g1", "k16")
    send["g2"][...] = mm(turn_c, recv["g1"][...].reshape(256, 128)).reshape(16, 16, 128)
    start("g2", "zc")
    share("u2_y", "y4", total("u2_z", "z"))
    s2_all = total("u2_y", "y4")
    s2 = jnp.where(first, s2_all[0:8], s2_all[8:16]) * mc2
    g2 = (zp2 - mm_t(s2, cr2)) * mh2
    r2 = z2 - mm_t(s2, V2)
    x2 = mm_t(r2, blk2[...]) + mm_t(g2, Q2)
    out2[...] = x2
    wait("g2", "zc")
    xu2 = t_mm(recv["g2"][...].reshape(256, 128), at2)[0:8]

    full2 = jnp.concatenate([x2, xu2], axis=1)
    vals = mm_t(full2, oh1)
    share("u1_xc", "xc", mm(jnp.where(front1, jnp.concatenate([vals, vals], axis=0), 0.0), c1h))
    send["h1"][...] = mm_t(oh1, stack16(full2)).reshape(8, 16, 128)
    start("h1", "k8")
    share("u1_z", "z", total("u1_xc", "xc"))
    wait("h1", "k8")
    send["h2"][...] = t_mm(turn_b, recv["h1"][...].reshape(128, 128)).reshape(16, 8, 128)
    start("h2", "zc")
    share("u1_y", "y2", total("u1_z", "z"))
    s1_all = total("u1_y", "y2")
    s1 = jnp.where(yb == 0, s1_all[0:8], s1_all[8:16]) * mc1
    g1 = (zp1 - mm_t(s1, cr1)) * mh1
    r1 = z1 - mm_t(s1, V1)
    x1 = mm_t(r1, blk1[...]) + mm_t(g1, Q1)
    out1[...] = x1
    wait("h2", "zc")
    xu1 = t_mm(recv["h2"][...].reshape(128, 128), at1)[0:8]

    vals = mm_t(jnp.concatenate([x1, xu1], axis=1), oh0)
    send["u0_zc"][...] = mm(jnp.where(front0, stack16(vals), 0.0), c0h).reshape(16, 8, 128)
    start("u0_zc", "zc")
    zp0 = total("zp0", "x")
    share("u0_x", "x", total("u0_zc", "zc"))
    s0 = total("u0_x", "x") * mc0
    g0 = (zp0 - mm_t(s0, cr0)) * mh0
    r0 = z0 - mm_t(s0, V0)
    out0[...] = mm_t(r0, blk0[...]) + mm_t(g0, Q0)

    for name, axis in pending:
        whole(name, axis).wait_send()


def shards(*args):
    args = list(args)
    for i in (4, 12, 20, 28):
        args[i] = args[i].reshape(1, -1)
    for i in (7, 15, 23):
        args[i] = args[i].reshape(1, -1)
    ranks = (6, 14, 22, 29)
    vmem = pl.BlockSpec(memory_space=pltpu.VMEM)
    smem = pl.BlockSpec(memory_space=pltpu.SMEM)
    sizes = {name: (n, rows, 128) for name, n, rows in EXCHANGES}
    scratch = [pltpu.VMEM(sizes[name], jnp.float32) for name in NAMES]
    scratch += [pltpu.VMEM(sizes[name], jnp.float32) for name in SCATTERED]
    scratch += [pltpu.SemaphoreType.DMA((len(NAMES),)), pltpu.SemaphoreType.DMA((len(NAMES),))]
    return tuple(
        pl.pallas_call(
            kernel,
            out_shape=[jax.ShapeDtypeStruct((8, 128), jnp.float32)] * 4,
            in_specs=[smem if i in ranks else vmem for i in range(len(args))],
            out_specs=[vmem] * 4,
            scratch_shapes=scratch,
            compiler_params=pltpu.CompilerParams(
                collective_id=0, has_side_effects=True, vmem_limit_bytes=48 * 1024 * 1024
            ),
            name="solve",
        )(*args)
    )


def solution(mesh):
    columns = P(None, ("leaf", "grid"))
    rows = P(("leaf", "grid"), None)
    flat = P(("leaf", "grid"))
    level = (columns, rows, rows, rows, flat, rows, P(), flat)
    in_specs = level * 3 + (columns, rows, rows, rows, flat, P())
    return jax.shard_map(
        shards, mesh=mesh, in_specs=in_specs, out_specs=(columns,) * 4, check_vma=False
    )
```

```python
import functools

import jax
import jax.numpy as jnp
from jax import lax
from jax.experimental import pallas as pl
from jax.experimental.pallas import tpu as pltpu
from jax.sharding import PartitionSpec as P

MESH = pl.DeviceIdType.MESH
HIGHEST = lax.Precision.HIGHEST

NX, NZC, NY = 4, 16, 4

EXCHANGES = [
    ("x0", 4, 144),
    ("zp0", 4, 8),
    ("w0", 16, 8),
    ("a1", 16, 24),
    ("a2", 4, 80),
    ("b1", 16, 16),
    ("b2", 8, 32),
    ("c1", 16, 24),
    ("c2", 16, 32),
    ("cr_xc", 8, 48),
    ("cr_z", 8, 48),
    ("cr_m", 8, 16),
    ("cr_y", 4, 32),
    ("cr_g", 8, 48),
    ("f1_xc", 8, 16),
    ("f1_z", 8, 16),
    ("f1_y", 2, 8),
    ("f2_xc", 8, 24),
    ("f2_z", 8, 24),
    ("f2_y", 4, 24),
    ("f3_xc", 8, 24),
    ("f3_z", 8, 24),
    ("f3_y", 4, 24),
    ("d1", 16, 8),
    ("d2", 8, 16),
    ("e1", 16, 16),
    ("e2", 16, 16),
    ("u2_xc", 8, 16),
    ("u2_z", 8, 16),
    ("u2_y", 4, 16),
    ("g1", 16, 16),
    ("g2", 16, 16),
    ("u1_xc", 8, 16),
    ("u1_z", 8, 16),
    ("u1_y", 2, 16),
    ("h1", 8, 16),
    ("h2", 16, 8),
    ("u0_zc", 16, 8),
    ("u0_x", 4, 8),
]
NAMES = [entry[0] for entry in EXCHANGES]
SCATTERED = ["a1", "a2", "b1", "b2", "c1", "c2", "cr_xc", "d1", "d2", "e1", "e2", "g1", "g2", "h1", "h2", "u0_zc"]


def dot(a, b, ca, cb):
    return lax.dot_general(
        a, b, (((ca,), (cb,)), ((), ())), precision=HIGHEST, preferred_element_type=jnp.float32
    )


def mm(a, b):
    return dot(a, b, 1, 0)


def mm_t(a, b):
    return dot(a, b, 1, 1)


def t_mm(a, b):
    return dot(a, b, 0, 0)


def iota(shape, dim):
    return lax.broadcasted_iota(jnp.int32, shape, dim)


def ones_where(cond):
    return jnp.where(cond, 1.0, 0.0).astype(jnp.float32)


def stack16(v):
    return jnp.concatenate([v] * 16, axis=0)


class Operand:
    def __init__(self, i, *refs):
        self.vmem = refs[31 + i]
        self.copy = pltpu.make_async_copy(refs[i], self.vmem, refs[-1].at[i])
        self.start = self.copy.start
        self.here = False

    def ready(self):
        if not self.here:
            self.copy.wait()
            self.here = True

    def __getitem__(self, index):
        self.ready()
        return self.vmem[index]

    def rank(self, side, front):
        if self.vmem.shape[1] == 2 and self.vmem.shape[0] < 3:
            column = self[:, side : side + 1].astype(jnp.float32)
            return jnp.sum(jnp.where(iota(column.shape, 0) == front, column, 0.0), axis=0, keepdims=True)
        row = self[side : side + 1, :].astype(jnp.float32)
        return jnp.sum(jnp.where(iota(row.shape, 1) == front, row, 0.0), axis=1, keepdims=True)


def kernel(*refs):
    (
        src0, blk0, exp0, bas0, piv0, cpl0, rnk0, tgt0,
        src1, blk1, exp1, bas1, piv1, cpl1, rnk1, tgt1,
        src2, blk2, exp2, bas2, piv2, cpl2, rnk2, tgt2,
        src3, blk3, exp3, bas3, piv3, rnk3,
        out,
    ) = [Operand(i, *refs) for i in range(30)] + list(refs[30:31])
    refs = refs[61:]
    n_ex = len(EXCHANGES)
    recv = dict(zip(NAMES, refs[:n_ex]))
    send = dict(zip(SCATTERED, refs[n_ex : n_ex + len(SCATTERED)]))
    send_sem, recv_sem = refs[n_ex + len(SCATTERED) : n_ex + len(SCATTERED) + 2]

    for operand in (tgt0, cpl0, src0, blk0, bas0, exp0):
        operand.start()

    leaf = lax.axis_index("leaf")
    x = lax.axis_index("grid")
    y = leaf // 16
    zc = leaf % 16
    z = zc // 2
    c = zc % 2
    u = y // 2
    yb = y % 2
    xc = x * 2 + c
    k8 = yb * 4 + x
    k16 = y * 4 + x

    axes = {
        "x": (x, 4, lambda d: (leaf, d)),
        "zc": (zc, 16, lambda d: (y * 16 + d, x)),
        "xc": (xc, 8, lambda d: (leaf - c + d % 2, d // 2)),
        "z": (z, 8, lambda d: (y * 16 + d * 2 + c, x)),
        "y2": (yb, 2, lambda d: ((u * 2 + d) * 16 + zc, x)),
        "y4": (y, 4, lambda d: (d * 16 + zc, x)),
        "k8": (k8, 8, lambda d: ((u * 2 + d // 4) * 16 + zc, d % 4)),
        "k16": (k16, 16, lambda d: ((d // 4) * 16 + zc, d % 4)),
    }
    pending = []

    def copy_of(name, src, dst, dev):
        i = NAMES.index(name)
        return pltpu.make_async_remote_copy(
            src_ref=src,
            dst_ref=dst,
            send_sem=send_sem.at[i],
            recv_sem=recv_sem.at[i],
            device_id=dev,
            device_id_type=MESH,
        )

    def start(name, axis):
        me, n, dev = axes[axis]
        buf = recv[name]
        scattered = name in send

        def body(o, carry):
            d = lax.rem(me + o, n)
            src = send[name].at[d] if scattered else buf.at[me]
            copy_of(name, src, buf.at[me], dev(d)).start()
            return carry

        if scattered:
            buf[me] = send[name][me]
        lax.fori_loop(1, n, body, 0)
        pending.append((name, axis))

    def whole(name, axis):
        me, n, dev = axes[axis]
        part = recv[name].at[pl.ds(0, n - 1)]
        return copy_of(name, part, part, dev(lax.rem(me + 1, n)))

    def wait(name, axis):
        whole(name, axis).wait_recv()

    def share(name, axis, value):
        recv[name][axes[axis][0]] = value
        start(name, axis)

    def total(name, axis):
        wait(name, axis)
        return jnp.sum(recv[name][...], axis=0)

    barrier = pltpu.get_barrier_semaphore()

    def greet(axis):
        me, n, dev = axes[axis]

        def body(o, carry):
            pl.semaphore_signal(barrier, inc=1, device_id=dev(lax.rem(me + o, n)), device_id_type=MESH)
            return carry

        lax.fori_loop(1, n, body, 0)
        return n - 1

    greeted = greet("zc") + greet("k16") + greet("xc")

    for operand in (
        exp1, bas1, exp2, bas2, exp3, piv3, rnk0, piv0, tgt1, cpl1, tgt2, cpl2, src1, blk1, rnk1, piv1,
        src2, blk2, rnk2, piv2, src3, blk3, bas3, rnk3,
    ):
        operand.start()

    lane = iota((1, 128), 1)

    def mask_of(ref, front, side):
        return ones_where(lane.astype(jnp.float32) < ref.rank(side, front))

    def column(row):
        n = row.shape[1]
        return jnp.transpose(jnp.broadcast_to(row, (128, n)))

    def packets(targets, sep_bits, kbits, ranked):
        piece = targets >> sep_bits
        within = targets & ((1 << sep_bits) - 1)
        label = piece * 128 + (within & 127) + 1
        owner = within >> 7
        if ranked:
            n = targets.shape[1]
            of = owner.astype(jnp.float32)
            same = column(of)[:, 0:1] == of
            before = iota((n, n), 0) < iota((n, n), 1)
            order = jnp.sum(ones_where(same & before), axis=0, keepdims=True)
            return of * 4.0 + order, label.astype(jnp.float32)
        sub = owner & 63
        pos = ((sub >> 2) << kbits) + ((owner >> 6) << 2) + (sub & 3)
        return pos.astype(jnp.float32), label.astype(jnp.float32)

    def place(pos, count):
        n = pos.shape[1]
        return ones_where(iota((count, n), 0).astype(jnp.float32) == pos)

    def label_rows(pos, label, kbits):
        n = pos.shape[1]
        ipos = pos.astype(jnp.int32)
        major = (ipos >> kbits).astype(jnp.float32)
        minor = (ipos & ((1 << kbits) - 1)).astype(jnp.float32)
        pick = ones_where(iota((16, n), 0).astype(jnp.float32) == major)
        spread = jnp.where(iota((n, 128), 1).astype(jnp.float32) == column(minor), column(label), 0.0)
        return mm(pick, spread)

    def fill_packets(name, pos, label, rows, kbits, couple):
        k = 1 << kbits
        at = place(pos, 16 * k)
        send[name][:, 0:k, :] = mm(at, couple).reshape(16, k, 128)
        lab = label_rows(pos, label, kbits)
        send[name][:, k : k + 8, :] = jnp.broadcast_to(lab[:, None, :], (16, 8, 128))
        return at

    pos0, lab0 = packets(tgt0[...], 13, 4, True)
    fill_packets("a1", pos0, lab0, 24, 4, cpl0[...])
    Q0, V0 = bas0[:, 0:128], bas0[:, 128:256]
    loc0 = mm(src0[...], blk0[...])
    x0_own = jnp.concatenate(
        [mm(src0[...], Q0), mm(loc0, V0), t_mm(exp0[...], V0)], axis=0
    )

    pl.semaphore_wait(barrier, greeted)
    share("x0", "x", x0_own)
    start("a1", "zc")

    V1 = bas1[:, 128:256]
    V2 = bas2[:, 128:256]
    cr1_own = t_mm(exp1[...], V1)
    cr2_own = t_mm(exp2[...], V2)
    P3 = exp3[...]
    scaled3 = P3 * column(piv3[...])
    m3_own = t_mm(P3, scaled3)
    send["cr_xc"][:, 0:16, :] = cr1_own.reshape(8, 16, 128)
    send["cr_xc"][:, 16:32, :] = cr2_own.reshape(8, 16, 128)
    send["cr_xc"][:, 32:48, :] = m3_own.reshape(8, 16, 128)
    start("cr_xc", "xc")

    mh0, mc0 = mask_of(rnk0, leaf, 0), mask_of(rnk0, leaf, 1)
    tot0 = total("x0", "x")
    hq0 = tot0[0:8] * mh0
    cr0 = tot0[16:144]
    w0 = (tot0[8:16] + mm(hq0, cr0)) * mc0
    share("w0", "zc", w0)
    z0 = (loc0 + mm_t(hq0, exp0[...])) * piv0[...]
    share("zp0", "x", mm(z0, exp0[...]))

    wait("a1", "zc")
    s_row = iota((256, 256), 0)
    r_col = iota((256, 256), 1)
    turn_a = ones_where(r_col == ((s_row >> 2) & 15) * 16 + (s_row >> 6) * 4 + (s_row & 3))
    moved = mm(turn_a, recv["a1"][:, 0:16, :].reshape(256, 128))
    labels = jnp.max(recv["a1"][:, 16:24, :], axis=1)
    send["a2"][:, 0:64, :] = moved.reshape(4, 64, 128)
    send["a2"][:, 64:80, :] = jnp.broadcast_to(labels[None], (4, 16, 128))
    start("a2", "x")

    cr_z_own = total("cr_xc", "xc")
    share("cr_z", "z", cr_z_own)

    pos1, lab1 = packets(tgt1[...], 14, 3, False)
    at1 = fill_packets("b1", pos1, lab1, 16, 3, cpl1[...])
    start("b1", "zc")
    pos2, lab2 = packets(tgt2[...], 15, 4, False)
    at2 = fill_packets("c1", pos2, lab2, 24, 4, cpl2[...])
    start("c1", "zc")

    wait("w0", "zc")
    wait("a2", "x")
    c0h = recv["a2"][:, 0:64, :].reshape(256, 128)
    lab_in = recv["a2"][:, 64:80, :].reshape(64, 128)
    spread = mm(ones_where(iota((256, 64), 1) == (iota((256, 64), 0) >> 2)), lab_in)
    mine = iota((256, 128), 1) == x * 4 + (iota((256, 128), 0) & 3)
    lab_col = jnp.sum(jnp.where(mine, spread, 0.0), axis=1, keepdims=True)
    oh0 = ones_where(iota((256, 256), 1).astype(jnp.float32) == lab_col - 1.0)
    front0 = (iota((128, 256), 0) >> 3) == ((iota((128, 256), 1) & 63) >> 2)
    e0 = jnp.where(front0, mm_t(recv["w0"][...].reshape(128, 128), c0h), 0.0)
    inc0 = -mm(jnp.sum(e0.reshape(16, 8, 256), axis=0), oh0)
    b1 = src1[...] + inc0[:, 0:128]
    upd1 = inc0[:, 128:256]
    loc1 = mm(b1, blk1[...])
    Q1 = bas1[:, 0:128]
    share("f1_xc", "xc", jnp.concatenate([mm(b1, Q1), mm(loc1, V1)], axis=0))
    send["d1"][...] = mm_t(at1, stack16(upd1)).reshape(16, 8, 128)
    start("d1", "zc")

    cr_sum = total("cr_z", "z")
    share("cr_m", "xc", cr_sum[0:16])
    share("cr_y", "y4", cr_sum[16:48])

    share("f1_z", "z", total("f1_xc", "xc"))

    wait("b1", "zc")
    turn_b = ones_where(iota((128, 128), 1) == (iota((128, 128), 0) & 15) * 8 + (iota((128, 128), 0) >> 4))
    send["b2"][:, 0:16, :] = mm(turn_b, recv["b1"][:, 0:8, :].reshape(128, 128)).reshape(8, 16, 128)
    send["b2"][:, 16:32, :] = jnp.broadcast_to(jnp.max(recv["b1"][:, 8:16, :], axis=1)[None], (8, 16, 128))
    start("b2", "k8")
    wait("d1", "zc")
    send["d2"][...] = mm(turn_b, recv["d1"][...].reshape(128, 128)).reshape(8, 16, 128)
    start("d2", "k8")
    wait("cr_y", "y4")
    cy = recv["cr_y"]
    share(
        "cr_g",
        "xc",
        jnp.concatenate(
            [
                cy[0, 0:16, :] + cy[1, 0:16, :],
                cy[2, 0:16, :] + cy[3, 0:16, :],
                (cy[0, 16:32, :] + cy[1, 16:32, :]) + (cy[2, 16:32, :] + cy[3, 16:32, :]),
            ],
            axis=0,
        ),
    )
    wait("c1", "zc")
    turn_c = ones_where(r_col == (s_row & 15) * 16 + (s_row >> 4))
    send["c2"][:, 0:16, :] = mm(turn_c, recv["c1"][:, 0:16, :].reshape(256, 128)).reshape(16, 16, 128)
    send["c2"][:, 16:32, :] = jnp.broadcast_to(jnp.max(recv["c1"][:, 16:24, :], axis=1)[None], (16, 16, 128))
    start("c2", "k16")

    wait("cr_m", "xc")
    cr1 = recv["cr_m"][...].reshape(128, 128)
    mh1, mc1 = mask_of(rnk1, y, 0), mask_of(rnk1, y, 1)
    tot1 = total("f1_z", "z")
    hq1 = tot1[0:8] * mh1
    share("f1_y", "y2", (tot1[8:16] + mm(hq1, cr1)) * mc1)
    z1 = (loc1 + mm_t(hq1, exp1[...])) * piv1[...]
    zp1_own = mm(z1, exp1[...])

    wait("b2", "k8")
    c1h = recv["b2"][:, 0:16, :].reshape(128, 128)
    lab_in = recv["b2"][:, 16:32, :].reshape(128, 128)
    lab_col = jnp.sum(jnp.where(iota((128, 128), 1) == k8, lab_in, 0.0), axis=1, keepdims=True)
    oh1 = ones_where(iota((128, 256), 1).astype(jnp.float32) == lab_col - 1.0)
    front1 = (iota((16, 128), 0) >> 3) == (iota((16, 128), 1) >> 6)
    wait("d2", "k8")
    came1 = jnp.transpose(recv["d2"][...].reshape(128, 128))[0:8]
    wait("f1_y", "y2")
    e1 = jnp.where(front1, mm_t(recv["f1_y"][...].reshape(16, 128), c1h), 0.0)
    inc1 = mm(came1 - (e1[0:8] + e1[8:16]), oh1)
    b2 = src2[...] + inc1[:, 0:128]
    upd2 = inc1[:, 128:256]
    loc2 = mm(b2, blk2[...])
    Q2 = bas2[:, 0:128]
    share("f2_xc", "xc", jnp.concatenate([mm(b2, Q2), mm(loc2, V2), zp1_own], axis=0))
    send["e1"][...] = mm_t(at2, stack16(upd2)).reshape(16, 16, 128)
    start("e1", "zc")
    share("f2_z", "z", total("f2_xc", "xc"))
    wait("e1", "zc")
    send["e2"][...] = mm(turn_c, recv["e1"][...].reshape(256, 128)).reshape(16, 16, 128)
    start("e2", "k16")
    wait("cr_g", "xc")
    cg = recv["cr_g"]
    cr2_each = [cg[:, 0:16, :].reshape(128, 128), cg[:, 16:32, :].reshape(128, 128)]
    m3 = cg[:, 32:48, :].reshape(128, 128)
    wait("c2", "k16")
    c2h = recv["c2"][:, 0:16, :].reshape(256, 128)
    lab_in = recv["c2"][:, 16:32, :].reshape(256, 128)
    lab_col = jnp.sum(jnp.where(iota((256, 128), 1) == k16, lab_in, 0.0), axis=1, keepdims=True)
    oh2 = ones_where(iota((256, 128), 1).astype(jnp.float32) == lab_col - 1.0)
    front2 = (iota((16, 256), 0) >> 3) == (iota((16, 256), 1) >> 7)
    share("f2_y", "y4", total("f2_z", "z"))
    wait("f2_y", "y4")
    fy = recv["f2_y"]
    hq2_each, w2_each = [], []
    for v in range(2):
        t1 = fy[2 * v, 0:8, :] + fy[2 * v + 1, 0:8, :]
        t2 = fy[2 * v, 8:16, :] + fy[2 * v + 1, 8:16, :]
        hq = t1 * mask_of(rnk2, v, 0)
        hq2_each.append(hq)
        w2_each.append((t2 + mm(hq, cr2_each[v])) * mask_of(rnk2, v, 1))
    zp1 = fy[y, 16:24, :]
    first = u == 0
    hq2 = jnp.where(first, hq2_each[0], hq2_each[1])
    cr2 = jnp.where(first, cr2_each[0], cr2_each[1])
    mh2, mc2 = mask_of(rnk2, u, 0), mask_of(rnk2, u, 1)
    z2 = (loc2 + mm_t(hq2, exp2[...])) * piv2[...]
    zp2_own = mm(z2, exp2[...])

    e2 = jnp.where(front2, mm_t(jnp.concatenate(w2_each, axis=0), c2h), 0.0)
    wait("e2", "k16")
    came2 = jnp.transpose(recv["e2"][...].reshape(256, 128))[0:8]
    b3 = src3[...] + mm(came2 - (e2[0:8] + e2[8:16]), oh2)
    loc3 = mm(b3, blk3[...])
    Q3 = bas3[:, 0:128]
    share("f3_xc", "xc", jnp.concatenate([mm(b3, Q3), mm(loc3 * piv3[...], P3), zp2_own], axis=0))
    share("f3_z", "z", total("f3_xc", "xc"))
    share("f3_y", "y4", total("f3_z", "z"))
    wait("f3_y", "y4")
    fy = recv["f3_y"]
    lower = fy[0] + fy[1]
    upper = fy[2] + fy[3]
    mh3 = mask_of(rnk3, 0, 0)
    both = lower + upper
    hq3 = both[0:8] * mh3
    zp2 = jnp.where(first, lower[16:24], upper[16:24])
    g3 = (both[8:16] + mm(hq3, m3)) * mh3
    z3 = (loc3 + mm_t(hq3, P3)) * piv3[...]
    x3 = mm_t(z3, blk3[...]) + mm_t(g3, Q3)
    out[3] = x3

    vals = mm_t(x3, oh2)
    share("u2_xc", "xc", mm(jnp.where(front2, jnp.concatenate([vals, vals], axis=0), 0.0), c2h))
    send["g1"][...] = mm_t(oh2, stack16(x3)).reshape(16, 16, 128)
    start("g1", "k16")
    share("u2_z", "z", total("u2_xc", "xc"))
    wait("g1", "k16")
    send["g2"][...] = mm(turn_c, recv["g1"][...].reshape(256, 128)).reshape(16, 16, 128)
    start("g2", "zc")
    share("u2_y", "y4", total("u2_z", "z"))
    s2_all = total("u2_y", "y4")
    s2 = jnp.where(first, s2_all[0:8], s2_all[8:16]) * mc2
    g2 = (zp2 - mm_t(s2, cr2)) * mh2
    r2 = z2 - mm_t(s2, V2)
    x2 = mm_t(r2, blk2[...]) + mm_t(g2, Q2)
    out[2] = x2
    wait("g2", "zc")
    xu2 = t_mm(recv["g2"][...].reshape(256, 128), at2)[0:8]

    full2 = jnp.concatenate([x2, xu2], axis=1)
    vals = mm_t(full2, oh1)
    share("u1_xc", "xc", mm(jnp.where(front1, jnp.concatenate([vals, vals], axis=0), 0.0), c1h))
    send["h1"][...] = mm_t(oh1, stack16(full2)).reshape(8, 16, 128)
    start("h1", "k8")
    share("u1_z", "z", total("u1_xc", "xc"))
    wait("h1", "k8")
    send["h2"][...] = t_mm(turn_b, recv["h1"][...].reshape(128, 128)).reshape(16, 8, 128)
    start("h2", "zc")
    share("u1_y", "y2", total("u1_z", "z"))
    s1_all = total("u1_y", "y2")
    s1 = jnp.where(yb == 0, s1_all[0:8], s1_all[8:16]) * mc1
    g1 = (zp1 - mm_t(s1, cr1)) * mh1
    r1 = z1 - mm_t(s1, V1)
    x1 = mm_t(r1, blk1[...]) + mm_t(g1, Q1)
    out[1] = x1
    wait("h2", "zc")
    xu1 = t_mm(recv["h2"][...].reshape(128, 128), at1)[0:8]

    vals = mm_t(jnp.concatenate([x1, xu1], axis=1), oh0)
    send["u0_zc"][...] = mm(jnp.where(front0, stack16(vals), 0.0), c0h).reshape(16, 8, 128)
    start("u0_zc", "zc")
    zp0 = total("zp0", "x")
    share("u0_x", "x", total("u0_zc", "zc"))
    s0 = total("u0_x", "x") * mc0
    g0 = (zp0 - mm_t(s0, cr0)) * mh0
    r0 = z0 - mm_t(s0, V0)
    out[0] = mm_t(r0, blk0[...]) + mm_t(g0, Q0)

    for name, axis in pending:
        whole(name, axis).wait_send()


def apart(answers, *refs):
    copies = [pltpu.make_async_copy(answers.at[k], refs[k], refs[4].at[k]) for k in range(4)]
    for copy in copies:
        copy.start()
    for copy in copies:
        copy.wait()


def shards(*args):
    args = list(args)
    for i in (4, 12, 20, 28):
        args[i] = args[i].reshape(1, -1)
    for i in (7, 15, 23):
        args[i] = args[i].reshape(1, -1)
    for i in (6, 14):
        args[i] = args[i].T
    hbm = pl.BlockSpec(memory_space=pltpu.HBM)
    vmem = pl.BlockSpec(memory_space=pltpu.VMEM)
    sizes = {name: (n, rows, 128) for name, n, rows in EXCHANGES}
    scratch = [pltpu.VMEM(arg.shape, arg.dtype) for arg in args]
    scratch += [pltpu.VMEM(sizes[name], jnp.float32) for name in NAMES]
    scratch += [pltpu.VMEM(sizes[name], jnp.float32) for name in SCATTERED]
    scratch += [pltpu.SemaphoreType.DMA((len(NAMES),)), pltpu.SemaphoreType.DMA((len(NAMES),))]
    scratch += [pltpu.SemaphoreType.DMA((len(args),))]
    answers = pl.pallas_call(
        kernel,
        out_shape=jax.ShapeDtypeStruct((4, 8, 128), jnp.float32),
        in_specs=[hbm] * len(args),
        out_specs=vmem,
        scratch_shapes=scratch,
        compiler_params=pltpu.CompilerParams(
            collective_id=0, has_side_effects=True, vmem_limit_bytes=67043328
        ),
        name="solve",
    )(*args)
    return tuple(
        pl.pallas_call(
            apart,
            out_shape=[jax.ShapeDtypeStruct((8, 128), jnp.float32)] * 4,
            in_specs=[vmem],
            out_specs=[hbm] * 4,
            scratch_shapes=[pltpu.SemaphoreType.DMA((4,))],
            name="apart",
        )(answers)
    )


def solution(mesh):
    columns = P(None, ("leaf", "grid"))
    rows = P(("leaf", "grid"), None)
    flat = P(("leaf", "grid"))
    level = (columns, rows, rows, rows, flat, rows, P(), flat)
    in_specs = level * 3 + (columns, rows, rows, rows, flat, P())
    return jax.shard_map(
        shards, mesh=mesh, in_specs=in_specs, out_specs=(columns,) * 4, check_vma=False
    )
```

```python
import functools

import jax
import jax.numpy as jnp
from jax import lax
from jax.experimental import pallas as pl
from jax.experimental.pallas import tpu as pltpu
from jax.sharding import PartitionSpec as P

MESH = pl.DeviceIdType.MESH
HIGHEST = lax.Precision.HIGHEST

NX, NZC, NY = 4, 16, 4

EXCHANGES = [
    ("x0a", 4, 8, 8),
    ("x0b", 4, 8, 8),
    ("x0c", 4, 128, 128),
    ("zp0", 4, 8, 8),
    ("w0", 16, 8, 8),
    ("a1", 16, 24, 17),
    ("a2", 4, 80, 80),
    ("b1", 16, 16, 9),
    ("b2", 8, 32, 32),
    ("c1", 16, 24, 17),
    ("c2", 16, 32, 32),
    ("q_xc", 8, 16, 16),
    ("q_z", 8, 16, 16),
    ("q_g", 8, 16, 16),
    ("r_xc", 8, 32, 32),
    ("r_z", 8, 32, 32),
    ("r_y", 4, 32, 32),
    ("r_g", 8, 48, 48),
    ("f1_xc", 8, 16, 16),
    ("f1_z", 8, 16, 16),
    ("f1_y", 2, 8, 8),
    ("f2_xc", 8, 24, 24),
    ("f2_z", 8, 24, 24),
    ("f2_y", 4, 24, 24),
    ("f3_xc", 8, 24, 24),
    ("f3_z", 8, 24, 24),
    ("f3_y", 4, 24, 24),
    ("d1", 16, 1, 1),
    ("d2", 8, 1, 1),
    ("e1", 16, 1, 1),
    ("e2", 16, 1, 1),
    ("u2_xc", 8, 16, 16),
    ("u2_z", 8, 16, 16),
    ("u2_y", 4, 16, 16),
    ("g1", 16, 1, 1),
    ("g2", 16, 1, 1),
    ("u1_xc", 8, 16, 16),
    ("u1_z", 8, 16, 16),
    ("u1_y", 2, 16, 16),
    ("h1", 8, 1, 1),
    ("h2", 16, 1, 1),
    ("u0_zc", 16, 8, 8),
    ("u0_x", 4, 8, 8),
]
NAMES = [entry[0] for entry in EXCHANGES]
SENT = {entry[0]: entry[3] for entry in EXCHANGES}
SCATTERED = [
    "a1", "a2", "b1", "b2", "c1", "c2", "q_xc", "r_xc", "d1", "d2", "e1", "e2", "g1", "g2", "h1", "h2", "u0_zc"
]


def dot(a, b, ca, cb):
    return lax.dot_general(
        a, b, (((ca,), (cb,)), ((), ())), precision=HIGHEST, preferred_element_type=jnp.float32
    )


def mm(a, b):
    return dot(a, b, 1, 0)


def mm_t(a, b):
    return dot(a, b, 1, 1)


def t_mm(a, b):
    return dot(a, b, 0, 0)


def iota(shape, dim):
    return lax.broadcasted_iota(jnp.int32, shape, dim)


def ones_where(cond):
    return jnp.where(cond, 1.0, 0.0).astype(jnp.float32)


def stack16(v):
    return jnp.concatenate([v] * 16, axis=0)


class Operand:
    def __init__(self, i, *refs):
        self.vmem = refs[31 + i]
        self.copy = pltpu.make_async_copy(refs[i], self.vmem, refs[-1].at[i])
        self.start = self.copy.start
        self.here = False

    def ready(self):
        if not self.here:
            self.copy.wait()
            self.here = True

    def __getitem__(self, index):
        self.ready()
        return self.vmem[index]

    def rank(self, side, front):
        if self.vmem.shape[1] == 2 and self.vmem.shape[0] < 3:
            column = self[:, side : side + 1].astype(jnp.float32)
            return jnp.sum(jnp.where(iota(column.shape, 0) == front, column, 0.0), axis=0, keepdims=True)
        row = self[side : side + 1, :].astype(jnp.float32)
        return jnp.sum(jnp.where(iota(row.shape, 1) == front, row, 0.0), axis=1, keepdims=True)


def kernel(*refs):
    (
        src0, blk0, exp0, bas0, piv0, cpl0, rnk0, tgt0,
        src1, blk1, exp1, bas1, piv1, cpl1, rnk1, tgt1,
        src2, blk2, exp2, bas2, piv2, cpl2, rnk2, tgt2,
        src3, blk3, exp3, bas3, piv3, rnk3,
        out,
    ) = [Operand(i, *refs) for i in range(30)] + list(refs[30:31])
    refs = refs[61:]
    n_ex = len(EXCHANGES)
    recv = dict(zip(NAMES, refs[:n_ex]))
    send = dict(zip(SCATTERED, refs[n_ex : n_ex + len(SCATTERED)]))
    send_sem, recv_sem = refs[n_ex + len(SCATTERED) : n_ex + len(SCATTERED) + 2]

    for operand in (tgt0, cpl0, src0, blk0, bas0, exp0):
        operand.start()

    leaf = lax.axis_index("leaf")
    x = lax.axis_index("grid")
    y = leaf // 16
    zc = leaf % 16
    z = zc // 2
    c = zc % 2
    u = y // 2
    yb = y % 2
    xc = x * 2 + c
    k8 = yb * 4 + x
    k16 = y * 4 + x

    axes = {
        "x": (x, 4, lambda d: (leaf, d)),
        "zc": (zc, 16, lambda d: (y * 16 + d, x)),
        "xc": (xc, 8, lambda d: (leaf - c + d % 2, d // 2)),
        "z": (z, 8, lambda d: (y * 16 + d * 2 + c, x)),
        "y2": (yb, 2, lambda d: ((u * 2 + d) * 16 + zc, x)),
        "y4": (y, 4, lambda d: (d * 16 + zc, x)),
        "k8": (k8, 8, lambda d: ((u * 2 + d // 4) * 16 + zc, d % 4)),
        "k16": (k16, 16, lambda d: ((d // 4) * 16 + zc, d % 4)),
    }
    pending = []

    def copy_of(name, src, dst, dev):
        i = NAMES.index(name)
        return pltpu.make_async_remote_copy(
            src_ref=src,
            dst_ref=dst,
            send_sem=send_sem.at[i],
            recv_sem=recv_sem.at[i],
            device_id=dev,
            device_id_type=MESH,
        )

    def start(name, axis):
        me, n, dev = axes[axis]
        buf = recv[name]
        scattered = name in send

        def body(o, carry):
            d = lax.rem(me + o, n)
            rows = pl.ds(0, SENT[name])
            src = send[name].at[d, rows] if scattered else buf.at[me, rows]
            copy_of(name, src, buf.at[me, rows], dev(d)).start()
            return carry

        if scattered:
            buf[me] = send[name][me]
        lax.fori_loop(1, n, body, 0)
        pending.append((name, axis))

    def whole(name, axis):
        me, n, dev = axes[axis]
        part = recv[name].at[pl.ds(0, n - 1), pl.ds(0, SENT[name])]
        return copy_of(name, part, part, dev(lax.rem(me + 1, n)))

    def wait(name, axis):
        whole(name, axis).wait_recv()

    def share(name, axis, value):
        recv[name][axes[axis][0]] = value
        start(name, axis)

    def total(name, axis):
        wait(name, axis)
        return jnp.sum(recv[name][...], axis=0)

    barrier = pltpu.get_barrier_semaphore()

    def greet(axis):
        me, n, dev = axes[axis]

        def body(o, carry):
            pl.semaphore_signal(barrier, inc=1, device_id=dev(lax.rem(me + o, n)), device_id_type=MESH)
            return carry

        lax.fori_loop(1, n, body, 0)
        return n - 1

    greeted = greet("zc") + greet("k16") + greet("xc")

    for operand in (
        exp1, bas1, exp2, bas2, exp3, piv3, rnk0, piv0, tgt1, cpl1, tgt2, cpl2, src1, blk1, rnk1, piv1,
        src2, blk2, rnk2, piv2, src3, blk3, bas3, rnk3,
    ):
        operand.start()

    lane = iota((1, 128), 1)

    def mask_of(ref, front, side):
        return ones_where(lane.astype(jnp.float32) < ref.rank(side, front))

    def column(row):
        n = row.shape[1]
        return jnp.transpose(jnp.broadcast_to(row, (128, n)))

    def packets(targets, sep_bits, kbits, ranked):
        piece = targets >> sep_bits
        within = targets & ((1 << sep_bits) - 1)
        label = piece * 128 + (within & 127) + 1
        owner = within >> 7
        if ranked:
            n = targets.shape[1]
            of = owner.astype(jnp.float32)
            same = column(of)[:, 0:1] == of
            before = iota((n, n), 0) < iota((n, n), 1)
            order = jnp.sum(ones_where(same & before), axis=0, keepdims=True)
            return of * 4.0 + order, label.astype(jnp.float32)
        sub = owner & 63
        pos = ((sub >> 2) << kbits) + ((owner >> 6) << 2) + (sub & 3)
        return pos.astype(jnp.float32), label.astype(jnp.float32)

    def place(pos, count):
        n = pos.shape[1]
        return ones_where(iota((count, n), 0).astype(jnp.float32) == pos)

    def halves(pos, kbits):
        ipos = pos.astype(jnp.int32)
        return (ipos >> kbits).astype(jnp.float32), (ipos & ((1 << kbits) - 1)).astype(jnp.float32)

    def fill_packets(name, pos, label, kbits, couple):
        k = 1 << kbits
        n = pos.shape[1]
        send[name][:, 0:k, :] = mm(place(pos, 16 * k), couple).reshape(16, k, 128)
        major, minor = halves(pos, kbits)
        pick = ones_where(iota((16, n), 0).astype(jnp.float32) == major)
        minor_col = column(minor)
        spread = jnp.where(iota((n, 128), 1).astype(jnp.float32) == minor_col, column(label), 0.0)
        labels = mm(pick, spread)
        send[name][:, k : k + 8, :] = jnp.broadcast_to(labels[:, None, :], (16, 8, 128))
        return pick, (iota((n, 128), 1) >> 3).astype(jnp.float32) == minor_col

    def chain(qv, w, p):
        return jnp.concatenate([qv, mm(w, p)], axis=1)

    fold = ones_where((iota((128, 128), 0) & 7) == (iota((128, 128), 1) & 7))

    def blocks_are(shape_rows, of_row):
        return (iota((shape_rows, 128), 1) >> 3) == of_row(iota((shape_rows, 128), 0))

    def values_up(name, update, pick, block):
        rows = jnp.where(block, jnp.transpose(stack16(update)), 0.0)
        send[name][...] = mm(pick, rows).reshape(16, 1, 128)
        start(name, "zc")

    def values_on(name, got, outer, inner, axis):
        bits = inner.bit_length() - 1
        rows = jnp.concatenate([recv[got][...].reshape(inner, 128)] * outer, axis=0)
        rows = jnp.where(blocks_are(outer * inner, lambda r: r >> bits), rows, 0.0)
        rows = jnp.where(blocks_are(outer * inner, lambda r: r & (inner - 1)), mm(rows, fold), 0.0)
        send[name][...] = jnp.sum(rows.reshape(outer, inner, 128), axis=1).reshape(outer, 1, 128)
        start(name, axis)

    def values_in(got, k):
        rows = jnp.broadcast_to(recv[got][...], (k, 16, 128)).reshape(k * 16, 128)
        rows = jnp.where(blocks_are(k * 16, lambda r: r & 15), rows, 0.0)
        return mm_t(fold[0:8], rows)

    def values_down(name, onehot, full, k, axis):
        rows = mm_t(onehot, stack16(full))
        rows = jnp.where(blocks_are(k * 16, lambda r: r & 15), rows, 0.0)
        send[name][...] = jnp.sum(rows.reshape(k, 16, 128), axis=1).reshape(k, 1, 128)
        start(name, axis)

    def values_back(got, pick, block):
        rows = t_mm(pick, recv[got][...].reshape(16, 128))
        return mm_t(fold[0:8], jnp.where(block, rows, 0.0))

    pos0, lab0 = packets(tgt0[...], 13, 4, True)
    fill_packets("a1", pos0, lab0, 4, cpl0[...])
    Q0, V0 = bas0[:, 0:128], bas0[:, 128:256]
    t0 = mm(src0[...], Q0)
    loc0 = mm(src0[...], blk0[...])

    pl.semaphore_wait(barrier, greeted)
    share("x0a", "x", t0)
    start("a1", "zc")

    mh0, mc0 = mask_of(rnk0, leaf, 0), mask_of(rnk0, leaf, 1)
    V1 = bas1[:, 128:256]
    send["q_xc"][...] = t_mm(exp1[...], V1).reshape(8, 16, 128)
    hq0 = total("x0a", "x") * mh0
    y0 = loc0 + mm_t(hq0, exp0[...])
    share("x0b", "x", mm(y0, V0))
    start("q_xc", "xc")
    z0 = y0 * piv0[...]
    QW1 = chain(bas1[:, 0:128], blk1[...], V1)
    t1_src = mm(src1[...], QW1)
    share("w0", "zc", total("x0b", "x") * mc0)
    share("zp0", "x", mm(z0, exp0[...]))

    s_row = iota((256, 256), 0)
    r_col = iota((256, 256), 1)
    turn_a = ones_where(r_col == ((s_row >> 2) & 15) * 16 + (s_row >> 6) * 4 + (s_row & 3))
    wait("a1", "zc")
    moved = mm(turn_a, recv["a1"][:, 0:16, :].reshape(256, 128))
    send["a2"][:, 0:64, :] = moved.reshape(4, 64, 128)
    send["a2"][:, 64:80, :] = jnp.broadcast_to(recv["a1"][:, 16:17, :].reshape(1, 16, 128), (4, 16, 128))
    start("a2", "x")
    share("q_z", "z", total("q_xc", "xc"))

    pos1, lab1 = packets(tgt1[...], 14, 3, False)
    pick1, block1 = fill_packets("b1", pos1, lab1, 3, cpl1[...])
    pos2, lab2 = packets(tgt2[...], 15, 4, False)
    pick2, block2 = fill_packets("c1", pos2, lab2, 4, cpl2[...])
    V2 = bas2[:, 128:256]
    P3 = exp3[...]
    send["r_xc"][:, 0:16, :] = t_mm(exp2[...], V2).reshape(8, 16, 128)
    send["r_xc"][:, 16:32, :] = t_mm(P3, P3 * column(piv3[...])).reshape(8, 16, 128)

    front0 = (iota((128, 256), 0) >> 3) == ((iota((128, 256), 1) & 63) >> 2)
    spread4 = ones_where(iota((256, 64), 1) == (iota((256, 64), 0) >> 2))
    mine = iota((256, 128), 1) == x * 4 + (iota((256, 128), 0) & 3)
    wait("w0", "zc")
    wait("a2", "x")
    c0h = recv["a2"][:, 0:64, :].reshape(256, 128)
    e0 = jnp.where(front0, mm_t(recv["w0"][...].reshape(128, 128), c0h), 0.0)
    spread = mm(spread4, recv["a2"][:, 64:80, :].reshape(64, 128))
    lab_col = jnp.sum(jnp.where(mine, spread, 0.0), axis=1, keepdims=True)
    oh0 = ones_where(iota((256, 256), 1).astype(jnp.float32) == lab_col - 1.0)
    inc0 = -mm(jnp.sum(e0.reshape(16, 8, 256), axis=0), oh0)
    t1 = t1_src + mm(inc0[:, 0:128], QW1)
    share("f1_xc", "xc", jnp.concatenate([t1[:, 0:128], t1[:, 128:256]], axis=0))
    values_up("d1", inc0[:, 128:256], pick1, block1)
    start("b1", "zc")
    loc1 = mm(src1[...] + inc0[:, 0:128], blk1[...])
    ohq0 = mm(oh0[:, 0:128], QW1)

    share("f1_z", "z", total("f1_xc", "xc"))
    start("c1", "zc")
    start("r_xc", "xc")
    QW2 = chain(bas2[:, 0:128], blk2[...], V2)
    t2_src = mm(src2[...], QW2)
    share("q_g", "xc", total("q_z", "z"))
    wait("d1", "zc")
    values_on("d2", "d1", 8, 16, "k8")
    wait("b1", "zc")
    turn_b = ones_where(iota((128, 128), 1) == (iota((128, 128), 0) & 15) * 8 + (iota((128, 128), 0) >> 4))
    send["b2"][:, 0:16, :] = mm(turn_b, recv["b1"][:, 0:8, :].reshape(128, 128)).reshape(8, 16, 128)
    send["b2"][:, 16:32, :] = jnp.broadcast_to(recv["b1"][:, 8:9, :].reshape(1, 16, 128), (8, 16, 128))
    start("b2", "k8")
    share("r_z", "z", total("r_xc", "xc"))

    mh1, mc1 = mask_of(rnk1, y, 0), mask_of(rnk1, y, 1)
    wait("q_g", "xc")
    cr1 = recv["q_g"][...].reshape(128, 128)
    tot1 = total("f1_z", "z")
    hq1 = tot1[0:8] * mh1
    share("f1_y", "y2", (tot1[8:16] + mm(hq1, cr1)) * mc1)
    z1 = (loc1 + mm_t(hq1, exp1[...])) * piv1[...]
    zp1_own = mm(z1, exp1[...])
    zeta1 = mm_t(z1, blk1[...])

    wait("b2", "k8")
    c1h = recv["b2"][:, 0:16, :].reshape(128, 128)
    lab_in = recv["b2"][:, 16:32, :].reshape(128, 128)
    lab_col = jnp.sum(jnp.where(iota((128, 128), 1) == k8, lab_in, 0.0), axis=1, keepdims=True)
    oh1 = ones_where(iota((128, 256), 1).astype(jnp.float32) == lab_col - 1.0)
    ohq1 = mm(oh1[:, 0:128], QW2)
    kl1 = jnp.concatenate([t_mm(c1h[0:64], ohq1[0:64]), t_mm(c1h[64:128], ohq1[64:128])], axis=0)
    wait("d2", "k8")
    came1 = values_in("d2", 8)
    t2_src = t2_src + mm(came1, ohq1)
    inc1_came = mm(came1, oh1)
    wait("f1_y", "y2")
    w1 = recv["f1_y"]
    t2 = t2_src - mm(jnp.concatenate([w1[0], w1[1]], axis=1), kl1)
    share("f2_xc", "xc", jnp.concatenate([t2[:, 0:128], t2[:, 128:256], zp1_own], axis=0))
    front1 = (iota((16, 128), 0) >> 3) == (iota((16, 128), 1) >> 6)
    e1 = jnp.where(front1, mm_t(recv["f1_y"][...].reshape(16, 128), c1h), 0.0)
    inc1 = inc1_came - mm(e1[0:8] + e1[8:16], oh1)
    values_up("e1", inc1[:, 128:256], pick2, block2)
    loc2 = mm(src2[...] + inc1[:, 0:128], blk2[...])
    wait("c1", "zc")
    turn_c = ones_where(r_col == (s_row & 15) * 16 + (s_row >> 4))
    send["c2"][:, 0:16, :] = mm(turn_c, recv["c1"][:, 0:16, :].reshape(256, 128)).reshape(16, 16, 128)
    send["c2"][:, 16:32, :] = jnp.broadcast_to(recv["c1"][:, 16:17, :].reshape(1, 16, 128), (16, 16, 128))
    share("f2_z", "z", total("f2_xc", "xc"))
    start("c2", "k16")
    share("r_y", "y4", total("r_z", "z"))
    QW3 = chain(bas3[:, 0:128], blk3[...] * piv3[...], P3)
    t3_src = mm(src3[...], QW3)
    wait("e1", "zc")
    values_on("e2", "e1", 16, 16, "k16")
    wait("r_y", "y4")
    ry = recv["r_y"]
    share(
        "r_g",
        "xc",
        jnp.concatenate(
            [
                ry[0, 0:16, :] + ry[1, 0:16, :],
                ry[2, 0:16, :] + ry[3, 0:16, :],
                (ry[0, 16:32, :] + ry[1, 16:32, :]) + (ry[2, 16:32, :] + ry[3, 16:32, :]),
            ],
            axis=0,
        ),
    )
    share("f2_y", "y4", total("f2_z", "z"))
    wait("c2", "k16")
    c2h = recv["c2"][:, 0:16, :].reshape(256, 128)
    lab_in = recv["c2"][:, 16:32, :].reshape(256, 128)
    lab_col = jnp.sum(jnp.where(iota((256, 128), 1) == k16, lab_in, 0.0), axis=1, keepdims=True)
    oh2 = ones_where(iota((256, 128), 1).astype(jnp.float32) == lab_col - 1.0)
    ohq2 = mm(oh2, QW3)
    kl2 = jnp.concatenate([t_mm(c2h[0:128], ohq2[0:128]), t_mm(c2h[128:256], ohq2[128:256])], axis=0)
    wait("r_g", "xc")
    rg = recv["r_g"]
    cr2_each = [rg[:, 0:16, :].reshape(128, 128), rg[:, 16:32, :].reshape(128, 128)]
    m3 = rg[:, 32:48, :].reshape(128, 128)
    wait("f2_y", "y4")
    fy = recv["f2_y"]
    hq2_each, w2_each = [], []
    for v in range(2):
        t_q = fy[2 * v, 0:8, :] + fy[2 * v + 1, 0:8, :]
        t_v = fy[2 * v, 8:16, :] + fy[2 * v + 1, 8:16, :]
        hq = t_q * mask_of(rnk2, v, 0)
        hq2_each.append(hq)
        w2_each.append((t_v + mm(hq, cr2_each[v])) * mask_of(rnk2, v, 1))
    zp1 = fy[y, 16:24, :]
    first = u == 0
    hq2 = jnp.where(first, hq2_each[0], hq2_each[1])
    cr2 = jnp.where(first, cr2_each[0], cr2_each[1])
    mh2, mc2 = mask_of(rnk2, u, 0), mask_of(rnk2, u, 1)
    z2 = (loc2 + mm_t(hq2, exp2[...])) * piv2[...]
    zp2_own = mm(z2, exp2[...])

    t3_w = mm(jnp.concatenate(w2_each, axis=1), kl2)
    front2 = (iota((16, 256), 0) >> 3) == (iota((16, 256), 1) >> 7)
    wait("e2", "k16")
    came2 = values_in("e2", 16)
    t3 = t3_src + mm(came2, ohq2) - t3_w
    share("f3_xc", "xc", jnp.concatenate([t3[:, 0:128], t3[:, 128:256], zp2_own], axis=0))
    e2 = jnp.where(front2, mm_t(jnp.concatenate(w2_each, axis=0), c2h), 0.0)
    b3 = src3[...] + mm(came2 - (e2[0:8] + e2[8:16]), oh2)
    loc3 = mm(b3, blk3[...])
    share("f3_z", "z", total("f3_xc", "xc"))
    zeta3 = mm_t(loc3 * piv3[...], blk3[...])
    vals = mm_t(zeta3, oh2)
    u2_own = mm(jnp.where(front2, jnp.concatenate([vals, vals], axis=0), 0.0), c2h)
    zeta2 = mm_t(z2, blk2[...])
    mh3 = mask_of(rnk3, 0, 0)
    share("x0c", "x", t_mm(exp0[...], V0))
    share("f3_y", "y4", total("f3_z", "z"))
    QW0 = chain(Q0, blk0[...], V0)
    wait("f3_y", "y4")
    fy = recv["f3_y"]
    lower = fy[0] + fy[1]
    upper = fy[2] + fy[3]
    both = lower + upper
    hq3 = both[0:8] * mh3
    zp2 = jnp.where(first, lower[16:24], upper[16:24])
    g3 = (both[8:16] + mm(hq3, m3)) * mh3
    gh3 = jnp.concatenate([g3, hq3], axis=1)

    u2_low = mm_t(gh3, kl2)
    share("u2_xc", "xc", u2_own + jnp.concatenate([u2_low[:, 0:128], u2_low[:, 128:256]], axis=0))
    x3 = zeta3 + mm_t(gh3, QW3)
    out[3] = x3
    values_down("g1", oh2, x3, 16, "k16")
    share("u2_z", "z", total("u2_xc", "xc"))
    vals = mm_t(zeta2, oh1[:, 0:128])
    wait("g1", "k16")
    values_on("g2", "g1", 16, 16, "zc")
    share("u2_y", "y4", total("u2_z", "z"))
    wait("g2", "zc")
    xu2 = values_back("g2", pick2, block2)
    vals = vals + mm_t(xu2, oh1[:, 128:256])
    u1_own = mm(jnp.where(front1, jnp.concatenate([vals, vals], axis=0), 0.0), c1h)
    s2_all = total("u2_y", "y4")
    s2 = jnp.where(first, s2_all[0:8], s2_all[8:16]) * mc2
    g2 = (zp2 - mm_t(s2, cr2)) * mh2
    gs2 = jnp.concatenate([g2, -s2], axis=1)

    u1_low = mm_t(gs2, kl1)
    share("u1_xc", "xc", u1_own + jnp.concatenate([u1_low[:, 0:128], u1_low[:, 128:256]], axis=0))
    x2 = zeta2 + mm_t(gs2, QW2)
    out[2] = x2
    values_down("h1", oh1, jnp.concatenate([x2, xu2], axis=1), 8, "k8")
    share("u1_z", "z", total("u1_xc", "xc"))
    vals = mm_t(zeta1, oh0[:, 0:128])
    cr0 = total("x0c", "x")
    zp0 = total("zp0", "x")
    zeta0 = mm_t(z0, blk0[...])
    wait("h1", "k8")
    values_on("h2", "h1", 16, 8, "zc")
    share("u1_y", "y2", total("u1_z", "z"))
    wait("h2", "zc")
    xu1 = values_back("h2", pick1, block1)
    vals = vals + mm_t(xu1, oh0[:, 128:256])
    s1_all = total("u1_y", "y2")
    s1 = jnp.where(yb == 0, s1_all[0:8], s1_all[8:16]) * mc1
    g1 = (zp1 - mm_t(s1, cr1)) * mh1
    gs1 = jnp.concatenate([g1, -s1], axis=1)

    vals = vals + mm_t(gs1, ohq0)
    send["u0_zc"][...] = mm(jnp.where(front0, stack16(vals), 0.0), c0h).reshape(16, 8, 128)
    start("u0_zc", "zc")
    out[1] = zeta1 + mm_t(gs1, QW1)
    share("u0_x", "x", total("u0_zc", "zc"))
    s0 = total("u0_x", "x") * mc0
    g0 = (zp0 - mm_t(s0, cr0)) * mh0
    out[0] = zeta0 + mm_t(jnp.concatenate([g0, -s0], axis=1), QW0)

    for name, axis in pending:
        whole(name, axis).wait_send()


def apart(answers, *refs):
    copies = [pltpu.make_async_copy(answers.at[k], refs[k], refs[4].at[k]) for k in range(4)]
    for copy in copies:
        copy.start()
    for copy in copies:
        copy.wait()


def shards(*args):
    args = list(args)
    for i in (4, 12, 20, 28):
        args[i] = args[i].reshape(1, -1)
    for i in (7, 15, 23):
        args[i] = args[i].reshape(1, -1)
    for i in (6, 14):
        args[i] = args[i].T
    hbm = pl.BlockSpec(memory_space=pltpu.HBM)
    vmem = pl.BlockSpec(memory_space=pltpu.VMEM)
    sizes = {name: (n, rows, 128) for name, n, rows, _ in EXCHANGES}
    scratch = [pltpu.VMEM(arg.shape, arg.dtype) for arg in args]
    scratch += [pltpu.VMEM(sizes[name], jnp.float32) for name in NAMES]
    scratch += [pltpu.VMEM(sizes[name], jnp.float32) for name in SCATTERED]
    scratch += [pltpu.SemaphoreType.DMA((len(NAMES),)), pltpu.SemaphoreType.DMA((len(NAMES),))]
    scratch += [pltpu.SemaphoreType.DMA((len(args),))]
    answers = pl.pallas_call(
        kernel,
        out_shape=jax.ShapeDtypeStruct((4, 8, 128), jnp.float32),
        in_specs=[hbm] * len(args),
        out_specs=vmem,
        scratch_shapes=scratch,
        compiler_params=pltpu.CompilerParams(
            collective_id=0, has_side_effects=True, vmem_limit_bytes=67043328
        ),
        name="solve",
    )(*args)
    return tuple(
        pl.pallas_call(
            apart,
            out_shape=[jax.ShapeDtypeStruct((8, 128), jnp.float32)] * 4,
            in_specs=[vmem],
            out_specs=[hbm] * 4,
            scratch_shapes=[pltpu.SemaphoreType.DMA((4,))],
            name="apart",
        )(answers)
    )


def solution(mesh):
    columns = P(None, ("leaf", "grid"))
    rows = P(("leaf", "grid"), None)
    flat = P(("leaf", "grid"))
    level = (columns, rows, rows, rows, flat, rows, P(), flat)
    in_specs = level * 3 + (columns, rows, rows, rows, flat, P())
    return jax.shard_map(
        shards, mesh=mesh, in_specs=in_specs, out_specs=(columns,) * 4, check_vma=False
    )
```

```python
import functools

import jax
import jax.numpy as jnp
from jax import lax
from jax.experimental import pallas as pl
from jax.experimental.pallas import tpu as pltpu
from jax.sharding import PartitionSpec as P

MESH = pl.DeviceIdType.MESH
PRECISION = lax.Precision.HIGH

NX, NZC, NY = 4, 16, 4

EXCHANGES = [
    ("x0a", 4, 8, 8),
    ("x0b", 4, 8, 8),
    ("x0c", 4, 128, 128),
    ("zp0", 4, 8, 8),
    ("w0", 16, 8, 8),
    ("a1", 16, 24, 17),
    ("a2", 4, 80, 80),
    ("b1", 16, 16, 9),
    ("b2", 8, 32, 32),
    ("c1", 16, 24, 17),
    ("c2", 16, 32, 32),
    ("q_xc", 8, 16, 16),
    ("q_z", 8, 16, 16),
    ("q_g", 8, 16, 16),
    ("r_xc", 8, 32, 32),
    ("r_z", 8, 32, 32),
    ("r_y", 4, 32, 32),
    ("r_g", 8, 48, 48),
    ("f1_xc", 8, 16, 16),
    ("f1_z", 8, 16, 16),
    ("f1_y", 2, 8, 8),
    ("f2_xc", 8, 16, 16),
    ("f2_z", 8, 16, 16),
    ("f2_y", 4, 16, 16),
    ("f3_c", 2, 8, 8),
    ("f3_k", 16, 8, 8),
    ("f3_z", 8, 8, 8),
    ("f3_g", 2, 8, 8),
    ("zp_xc", 8, 16, 16),
    ("zp_z", 8, 16, 16),
    ("zp_y", 2, 8, 8),
    ("d1", 16, 1, 1),
    ("d2", 8, 1, 1),
    ("e1", 16, 1, 1),
    ("e2", 16, 1, 1),
    ("u2_c", 2, 8, 8),
    ("u2_k", 16, 8, 8),
    ("u2_z", 8, 8, 8),
    ("u2_g", 2, 8, 8),
    ("g1", 16, 1, 1),
    ("g2", 16, 1, 1),
    ("u1_xc", 8, 16, 16),
    ("u1_z", 8, 16, 16),
    ("u1_y", 2, 16, 16),
    ("h1", 8, 1, 1),
    ("h2", 16, 1, 1),
    ("u0_zc", 16, 8, 8),
    ("u0_x", 4, 8, 8),
]
NAMES = [entry[0] for entry in EXCHANGES]
SENT = {entry[0]: entry[3] for entry in EXCHANGES}
SCATTERED = [
    "a1", "a2", "b1", "b2", "c1", "c2", "q_xc", "r_xc", "d1", "d2", "e1", "e2", "f3_c", "u2_c", "g1", "g2", "h1", "h2", "u0_zc"
]


def dot(a, b, ca, cb):
    return lax.dot_general(
        a, b, (((ca,), (cb,)), ((), ())), precision=PRECISION, preferred_element_type=jnp.float32
    )


def mm(a, b):
    return dot(a, b, 1, 0)


def mm_t(a, b):
    return dot(a, b, 1, 1)


def t_mm(a, b):
    return dot(a, b, 0, 0)


def iota(shape, dim):
    return lax.broadcasted_iota(jnp.int32, shape, dim)


def ones_where(cond):
    return jnp.where(cond, 1.0, 0.0).astype(jnp.float32)


def stack16(v):
    return jnp.concatenate([v] * 16, axis=0)


class Operand:
    def __init__(self, i, *refs):
        self.vmem = refs[31 + i]
        self.copy = pltpu.make_async_copy(refs[i], self.vmem, refs[-1].at[i])
        self.start = self.copy.start
        self.here = False

    def ready(self):
        if not self.here:
            self.copy.wait()
            self.here = True

    def __getitem__(self, index):
        self.ready()
        return self.vmem[index]

    def rank(self, side, front):
        if self.vmem.shape[1] == 2 and self.vmem.shape[0] < 3:
            column = self[:, side : side + 1].astype(jnp.float32)
            return jnp.sum(jnp.where(iota(column.shape, 0) == front, column, 0.0), axis=0, keepdims=True)
        row = self[side : side + 1, :].astype(jnp.float32)
        return jnp.sum(jnp.where(iota(row.shape, 1) == front, row, 0.0), axis=1, keepdims=True)


def kernel(*refs):
    (
        src0, blk0, exp0, bas0, piv0, cpl0, rnk0, tgt0,
        src1, blk1, exp1, bas1, piv1, cpl1, rnk1, tgt1,
        src2, blk2, exp2, bas2, piv2, cpl2, rnk2, tgt2,
        src3, blk3, exp3, bas3, piv3, rnk3,
        out,
    ) = [Operand(i, *refs) for i in range(30)] + list(refs[30:31])
    refs = refs[61:]
    n_ex = len(EXCHANGES)
    recv = dict(zip(NAMES, refs[:n_ex]))
    send = dict(zip(SCATTERED, refs[n_ex : n_ex + len(SCATTERED)]))
    send_sem, recv_sem = refs[n_ex + len(SCATTERED) : n_ex + len(SCATTERED) + 2]

    for operand in (tgt0, cpl0, src0, blk0, bas0, exp0):
        operand.start()

    leaf = lax.axis_index("leaf")
    x = lax.axis_index("grid")
    y = leaf // 16
    zc = leaf % 16
    z = zc // 2
    c = zc % 2
    u = y // 2
    yb = y % 2
    xc = x * 2 + c
    k8 = yb * 4 + x
    k16 = y * 4 + x

    axes = {
        "x": (x, 4, lambda d: (leaf, d)),
        "zc": (zc, 16, lambda d: (y * 16 + d, x)),
        "xc": (xc, 8, lambda d: (leaf - c + d % 2, d // 2)),
        "c": (c, 2, lambda d: (leaf - c + d, x)),
        "z": (z, 8, lambda d: (y * 16 + d * 2 + c, x)),
        "y2": (yb, 2, lambda d: ((u * 2 + d) * 16 + zc, x)),
        "y4": (y, 4, lambda d: (d * 16 + zc, x)),
        "k8": (k8, 8, lambda d: ((u * 2 + d // 4) * 16 + zc, d % 4)),
        "k16": (k16, 16, lambda d: ((d // 4) * 16 + zc, d % 4)),
    }
    pending = []

    def copy_of(name, src, dst, dev):
        i = NAMES.index(name)
        return pltpu.make_async_remote_copy(
            src_ref=src,
            dst_ref=dst,
            send_sem=send_sem.at[i],
            recv_sem=recv_sem.at[i],
            device_id=dev,
            device_id_type=MESH,
        )

    def start(name, axis):
        me, n, dev = axes[axis]
        buf = recv[name]
        scattered = name in send

        def body(o, carry):
            d = lax.rem(me + o, n)
            rows = pl.ds(0, SENT[name])
            src = send[name].at[d, rows] if scattered else buf.at[me, rows]
            copy_of(name, src, buf.at[me, rows], dev(d)).start()
            return carry

        if scattered:
            buf[me] = send[name][me]
        lax.fori_loop(1, n, body, 0)
        pending.append((name, axis))

    def whole(name, axis):
        me, n, dev = axes[axis]
        part = recv[name].at[pl.ds(0, n - 1), pl.ds(0, SENT[name])]
        return copy_of(name, part, part, dev(lax.rem(me + 1, n)))

    def wait(name, axis):
        whole(name, axis).wait_recv()

    def share(name, axis, value):
        recv[name][axes[axis][0]] = value
        start(name, axis)

    def total(name, axis):
        wait(name, axis)
        return jnp.sum(recv[name][...], axis=0)

    def scatter_halves(name, low, high):
        send[name][0] = low
        send[name][1] = high
        start(name, "c")

    barrier = pltpu.get_barrier_semaphore()

    def greet(axis):
        me, n, dev = axes[axis]

        def body(o, carry):
            pl.semaphore_signal(barrier, inc=1, device_id=dev(lax.rem(me + o, n)), device_id_type=MESH)
            return carry

        lax.fori_loop(1, n, body, 0)
        return n - 1

    greeted = greet("zc") + greet("k16") + greet("xc")

    for operand in (
        exp1, bas1, exp2, bas2, exp3, piv3, rnk0, piv0, tgt1, cpl1, tgt2, cpl2, src1, blk1, rnk1, piv1,
        src2, blk2, rnk2, piv2, src3, blk3, bas3, rnk3,
    ):
        operand.start()

    lane = iota((1, 128), 1)

    def mask_of(ref, front, side):
        return ones_where(lane.astype(jnp.float32) < ref.rank(side, front))

    def column(row):
        n = row.shape[1]
        return jnp.transpose(jnp.broadcast_to(row, (128, n)))

    def packets(targets, sep_bits, kbits, ranked):
        piece = targets >> sep_bits
        within = targets & ((1 << sep_bits) - 1)
        label = piece * 128 + (within & 127) + 1
        owner = within >> 7
        if ranked:
            n = targets.shape[1]
            of = owner.astype(jnp.float32)
            same = column(of)[:, 0:1] == of
            before = iota((n, n), 0) < iota((n, n), 1)
            order = jnp.sum(ones_where(same & before), axis=0, keepdims=True)
            return of * 4.0 + order, label.astype(jnp.float32)
        sub = owner & 63
        pos = ((sub >> 2) << kbits) + ((owner >> 6) << 2) + (sub & 3)
        return pos.astype(jnp.float32), label.astype(jnp.float32)

    def place(pos, count):
        n = pos.shape[1]
        return ones_where(iota((count, n), 0).astype(jnp.float32) == pos)

    def halves(pos, kbits):
        ipos = pos.astype(jnp.int32)
        return (ipos >> kbits).astype(jnp.float32), (ipos & ((1 << kbits) - 1)).astype(jnp.float32)

    def fill_packets(name, pos, label, kbits, couple):
        k = 1 << kbits
        n = pos.shape[1]
        send[name][:, 0:k, :] = mm(place(pos, 16 * k), couple).reshape(16, k, 128)
        major, minor = halves(pos, kbits)
        pick = ones_where(iota((16, n), 0).astype(jnp.float32) == major)
        minor_col = column(minor)
        spread = jnp.where(iota((n, 128), 1).astype(jnp.float32) == minor_col, column(label), 0.0)
        labels = mm(pick, spread)
        send[name][:, k : k + 8, :] = jnp.broadcast_to(labels[:, None, :], (16, 8, 128))
        return pick, (iota((n, 128), 1) >> 3).astype(jnp.float32) == minor_col

    def chain(qv, w, p):
        return jnp.concatenate([qv, mm(w, p)], axis=1)

    fold = ones_where((iota((128, 128), 0) & 7) == (iota((128, 128), 1) & 7))

    def blocks_are(shape_rows, of_row):
        return (iota((shape_rows, 128), 1) >> 3) == of_row(iota((shape_rows, 128), 0))

    def values_up(name, update, pick, block):
        rows = jnp.where(block, jnp.transpose(stack16(update)), 0.0)
        send[name][...] = mm(pick, rows).reshape(16, 1, 128)
        start(name, "zc")

    def values_on(name, got, outer, inner, axis):
        bits = inner.bit_length() - 1
        rows = jnp.concatenate([recv[got][...].reshape(inner, 128)] * outer, axis=0)
        rows = jnp.where(blocks_are(outer * inner, lambda r: r >> bits), rows, 0.0)
        rows = jnp.where(blocks_are(outer * inner, lambda r: r & (inner - 1)), mm(rows, fold), 0.0)
        send[name][...] = jnp.sum(rows.reshape(outer, inner, 128), axis=1).reshape(outer, 1, 128)
        start(name, axis)

    def values_in(got, k):
        rows = jnp.broadcast_to(recv[got][...], (k, 16, 128)).reshape(k * 16, 128)
        rows = jnp.where(blocks_are(k * 16, lambda r: r & 15), rows, 0.0)
        return mm_t(fold[0:8], rows)

    def values_down(name, onehot, full, k, axis):
        rows = mm_t(onehot, stack16(full))
        rows = jnp.where(blocks_are(k * 16, lambda r: r & 15), rows, 0.0)
        send[name][...] = jnp.sum(rows.reshape(k, 16, 128), axis=1).reshape(k, 1, 128)
        start(name, axis)

    def values_back(got, pick, block):
        rows = t_mm(pick, recv[got][...].reshape(16, 128))
        return mm_t(fold[0:8], jnp.where(block, rows, 0.0))

    pos0, lab0 = packets(tgt0[...], 13, 4, True)
    fill_packets("a1", pos0, lab0, 4, cpl0[...])
    Q0, V0 = bas0[:, 0:128], bas0[:, 128:256]
    t0 = mm(src0[...], Q0)
    loc0 = mm(src0[...], blk0[...])

    pl.semaphore_wait(barrier, greeted)
    share("x0a", "x", t0)
    start("a1", "zc")

    mh0, mc0 = mask_of(rnk0, leaf, 0), mask_of(rnk0, leaf, 1)
    V1 = bas1[:, 128:256]
    send["q_xc"][...] = t_mm(exp1[...], V1).reshape(8, 16, 128)
    hq0 = total("x0a", "x") * mh0
    y0 = loc0 + mm_t(hq0, exp0[...])
    share("x0b", "x", mm(y0, V0))
    start("q_xc", "xc")
    z0 = y0 * piv0[...]
    QW1 = chain(bas1[:, 0:128], blk1[...], V1)
    t1_src = mm(src1[...], QW1)
    share("w0", "zc", total("x0b", "x") * mc0)
    share("zp0", "x", mm(z0, exp0[...]))

    s_row = iota((256, 256), 0)
    r_col = iota((256, 256), 1)
    turn_a = ones_where(r_col == ((s_row >> 2) & 15) * 16 + (s_row >> 6) * 4 + (s_row & 3))
    wait("a1", "zc")
    moved = mm(turn_a, recv["a1"][:, 0:16, :].reshape(256, 128))
    send["a2"][:, 0:64, :] = moved.reshape(4, 64, 128)
    send["a2"][:, 64:80, :] = jnp.broadcast_to(recv["a1"][:, 16:17, :].reshape(1, 16, 128), (4, 16, 128))
    start("a2", "x")
    share("q_z", "z", total("q_xc", "xc"))

    pos1, lab1 = packets(tgt1[...], 14, 3, False)
    pick1, block1 = fill_packets("b1", pos1, lab1, 3, cpl1[...])
    pos2, lab2 = packets(tgt2[...], 15, 4, False)
    pick2, block2 = fill_packets("c1", pos2, lab2, 4, cpl2[...])
    V2 = bas2[:, 128:256]
    P3 = exp3[...]
    send["r_xc"][:, 0:16, :] = t_mm(exp2[...], V2).reshape(8, 16, 128)
    send["r_xc"][:, 16:32, :] = t_mm(P3, P3 * column(piv3[...])).reshape(8, 16, 128)

    front0 = (iota((128, 256), 0) >> 3) == ((iota((128, 256), 1) & 63) >> 2)
    spread4 = ones_where(iota((256, 64), 1) == (iota((256, 64), 0) >> 2))
    mine = iota((256, 128), 1) == x * 4 + (iota((256, 128), 0) & 3)
    wait("w0", "zc")
    wait("a2", "x")
    c0h = recv["a2"][:, 0:64, :].reshape(256, 128)
    e0 = jnp.where(front0, mm_t(recv["w0"][...].reshape(128, 128), c0h), 0.0)
    spread = mm(spread4, recv["a2"][:, 64:80, :].reshape(64, 128))
    lab_col = jnp.sum(jnp.where(mine, spread, 0.0), axis=1, keepdims=True)
    oh0 = ones_where(iota((256, 256), 1).astype(jnp.float32) == lab_col - 1.0)
    inc0 = -mm(jnp.sum(e0.reshape(16, 8, 256), axis=0), oh0)
    t1 = t1_src + mm(inc0[:, 0:128], QW1)
    share("f1_xc", "xc", jnp.concatenate([t1[:, 0:128], t1[:, 128:256]], axis=0))
    values_up("d1", inc0[:, 128:256], pick1, block1)
    start("b1", "zc")
    loc1 = mm(src1[...] + inc0[:, 0:128], blk1[...])
    ohq0 = mm(oh0[:, 0:128], QW1)

    share("f1_z", "z", total("f1_xc", "xc"))
    start("c1", "zc")
    start("r_xc", "xc")
    QW2 = chain(bas2[:, 0:128], blk2[...], V2)
    t2_src = mm(src2[...], QW2)
    share("q_g", "xc", total("q_z", "z"))
    wait("d1", "zc")
    values_on("d2", "d1", 8, 16, "k8")
    wait("b1", "zc")
    turn_b = ones_where(iota((128, 128), 1) == (iota((128, 128), 0) & 15) * 8 + (iota((128, 128), 0) >> 4))
    send["b2"][:, 0:16, :] = mm(turn_b, recv["b1"][:, 0:8, :].reshape(128, 128)).reshape(8, 16, 128)
    send["b2"][:, 16:32, :] = jnp.broadcast_to(recv["b1"][:, 8:9, :].reshape(1, 16, 128), (8, 16, 128))
    start("b2", "k8")
    QW3 = chain(bas3[:, 0:128], blk3[...] * piv3[...], P3)
    t3_src = mm(src3[...], QW3)
    turn_c = ones_where(r_col == (s_row & 15) * 16 + (s_row >> 4))
    share("r_z", "z", total("r_xc", "xc"))

    mh1, mc1 = mask_of(rnk1, y, 0), mask_of(rnk1, y, 1)
    wait("q_g", "xc")
    cr1 = recv["q_g"][...].reshape(128, 128)
    tot1 = total("f1_z", "z")
    hq1 = tot1[0:8] * mh1
    share("f1_y", "y2", (tot1[8:16] + mm(hq1, cr1)) * mc1)
    z1 = (loc1 + mm_t(hq1, exp1[...])) * piv1[...]
    zp1_own = mm(z1, exp1[...])
    zeta1 = mm_t(z1, blk1[...])

    wait("b2", "k8")
    c1h = recv["b2"][:, 0:16, :].reshape(128, 128)
    lab_in = recv["b2"][:, 16:32, :].reshape(128, 128)
    lab_col = jnp.sum(jnp.where(iota((128, 128), 1) == k8, lab_in, 0.0), axis=1, keepdims=True)
    oh1 = ones_where(iota((128, 256), 1).astype(jnp.float32) == lab_col - 1.0)
    ohq1 = mm(oh1[:, 0:128], QW2)
    kl1 = jnp.concatenate([t_mm(c1h[0:64], ohq1[0:64]), t_mm(c1h[64:128], ohq1[64:128])], axis=0)
    wait("d2", "k8")
    came1 = values_in("d2", 8)
    t2_src = t2_src + mm(came1, ohq1)
    inc1_came = mm(came1, oh1)
    wait("f1_y", "y2")
    w1 = recv["f1_y"]
    t2 = t2_src - mm(jnp.concatenate([w1[0], w1[1]], axis=1), kl1)
    share("f2_xc", "xc", jnp.concatenate([t2[:, 0:128], t2[:, 128:256]], axis=0))
    front1 = (iota((16, 128), 0) >> 3) == (iota((16, 128), 1) >> 6)
    e1 = jnp.where(front1, mm_t(recv["f1_y"][...].reshape(16, 128), c1h), 0.0)
    inc1 = inc1_came - mm(e1[0:8] + e1[8:16], oh1)
    values_up("e1", inc1[:, 128:256], pick2, block2)
    loc2 = mm(src2[...] + inc1[:, 0:128], blk2[...])
    wait("c1", "zc")
    send["c2"][:, 0:16, :] = mm(turn_c, recv["c1"][:, 0:16, :].reshape(256, 128)).reshape(16, 16, 128)
    send["c2"][:, 16:32, :] = jnp.broadcast_to(recv["c1"][:, 16:17, :].reshape(1, 16, 128), (16, 16, 128))
    start("c2", "k16")
    share("r_y", "y4", total("r_z", "z"))
    share("f2_z", "z", total("f2_xc", "xc"))
    wait("e1", "zc")
    values_on("e2", "e1", 16, 16, "k16")
    wait("r_y", "y4")
    ry = recv["r_y"]
    share(
        "r_g",
        "xc",
        jnp.concatenate(
            [
                ry[0, 0:16, :] + ry[1, 0:16, :],
                ry[2, 0:16, :] + ry[3, 0:16, :],
                (ry[0, 16:32, :] + ry[1, 16:32, :]) + (ry[2, 16:32, :] + ry[3, 16:32, :]),
            ],
            axis=0,
        ),
    )
    share("f2_y", "y4", total("f2_z", "z"))
    wait("c2", "k16")
    c2h = recv["c2"][:, 0:16, :].reshape(256, 128)
    lab_in = recv["c2"][:, 16:32, :].reshape(256, 128)
    lab_col = jnp.sum(jnp.where(iota((256, 128), 1) == k16, lab_in, 0.0), axis=1, keepdims=True)
    oh2 = ones_where(iota((256, 128), 1).astype(jnp.float32) == lab_col - 1.0)
    ohq2 = mm(oh2, QW3)
    kl2 = jnp.concatenate([t_mm(c2h[0:128], ohq2[0:128]), t_mm(c2h[128:256], ohq2[128:256])], axis=0)
    wait("r_g", "xc")
    rg = recv["r_g"]
    cr2_each = [rg[:, 0:16, :].reshape(128, 128), rg[:, 16:32, :].reshape(128, 128)]
    m3 = rg[:, 32:48, :].reshape(128, 128)
    wait("f2_y", "y4")
    fy = recv["f2_y"]
    hq2_each, w2_each = [], []
    for v in range(2):
        t_q = fy[2 * v, 0:8, :] + fy[2 * v + 1, 0:8, :]
        t_v = fy[2 * v, 8:16, :] + fy[2 * v + 1, 8:16, :]
        hq = t_q * mask_of(rnk2, v, 0)
        hq2_each.append(hq)
        w2_each.append((t_v + mm(hq, cr2_each[v])) * mask_of(rnk2, v, 1))
    first = u == 0
    hq2 = jnp.where(first, hq2_each[0], hq2_each[1])
    cr2 = jnp.where(first, cr2_each[0], cr2_each[1])
    mh2, mc2 = mask_of(rnk2, u, 0), mask_of(rnk2, u, 1)
    z2 = (loc2 + mm_t(hq2, exp2[...])) * piv2[...]
    zp2_own = mm(z2, exp2[...])

    t3_w = mm(jnp.concatenate(w2_each, axis=1), kl2)
    front2 = (iota((16, 256), 0) >> 3) == (iota((16, 256), 1) >> 7)
    wait("e2", "k16")
    came2 = values_in("e2", 16)
    t3 = t3_src + mm(came2, ohq2) - t3_w
    scatter_halves("f3_c", t3[:, 0:128], t3[:, 128:256])
    share("zp_xc", "xc", jnp.concatenate([zp1_own, zp2_own], axis=0))
    share("f3_k", "k16", total("f3_c", "c"))
    e2 = jnp.where(front2, mm_t(jnp.concatenate(w2_each, axis=0), c2h), 0.0)
    b3 = src3[...] + mm(came2 - (e2[0:8] + e2[8:16]), oh2)
    loc3 = mm(b3, blk3[...])
    zeta3 = mm_t(loc3 * piv3[...], blk3[...])
    vals = mm_t(zeta3, oh2)
    u2_own = mm(jnp.where(front2, jnp.concatenate([vals, vals], axis=0), 0.0), c2h)
    share("f3_z", "z", total("f3_k", "k16"))
    zeta2 = mm_t(z2, blk2[...])
    mh3 = mask_of(rnk3, 0, 0)
    zp_sum = total("zp_xc", "xc")
    QW0 = chain(Q0, blk0[...], V0)
    share("f3_g", "c", total("f3_z", "z"))
    share("zp_z", "z", zp_sum)
    wait("f3_g", "c")
    hq3 = recv["f3_g"][0] * mh3
    g3 = (recv["f3_g"][1] + mm(hq3, m3)) * mh3
    gh3 = jnp.concatenate([g3, hq3], axis=1)

    u2_low = mm_t(gh3, kl2)
    scatter_halves("u2_c", u2_own[0:8] + u2_low[:, 0:128], u2_own[8:16] + u2_low[:, 128:256])
    x3 = zeta3 + mm_t(gh3, QW3)
    share("u2_k", "k16", total("u2_c", "c"))
    values_down("g1", oh2, x3, 16, "k16")
    out[3] = x3
    vals = mm_t(zeta2, oh1[:, 0:128])
    share("x0c", "x", t_mm(exp0[...], V0))
    share("u2_z", "z", total("u2_k", "k16"))
    wait("g1", "k16")
    values_on("g2", "g1", 16, 16, "zc")
    zp_sum = total("zp_z", "z")
    zp1 = zp_sum[0:8]
    share("zp_y", "y2", zp_sum[8:16])
    share("u2_g", "c", total("u2_z", "z"))
    zp2 = total("zp_y", "y2")
    wait("g2", "zc")
    xu2 = values_back("g2", pick2, block2)
    vals = vals + mm_t(xu2, oh1[:, 128:256])
    u1_own = mm(jnp.where(front1, jnp.concatenate([vals, vals], axis=0), 0.0), c1h)
    wait("u2_g", "c")
    s2 = recv["u2_g"][u] * mc2
    g2 = (zp2 - mm_t(s2, cr2)) * mh2
    gs2 = jnp.concatenate([g2, -s2], axis=1)

    u1_low = mm_t(gs2, kl1)
    share("u1_xc", "xc", u1_own + jnp.concatenate([u1_low[:, 0:128], u1_low[:, 128:256]], axis=0))
    x2 = zeta2 + mm_t(gs2, QW2)
    out[2] = x2
    values_down("h1", oh1, jnp.concatenate([x2, xu2], axis=1), 8, "k8")
    share("u1_z", "z", total("u1_xc", "xc"))
    vals = mm_t(zeta1, oh0[:, 0:128])
    cr0 = total("x0c", "x")
    zp0 = total("zp0", "x")
    zeta0 = mm_t(z0, blk0[...])
    wait("h1", "k8")
    values_on("h2", "h1", 16, 8, "zc")
    share("u1_y", "y2", total("u1_z", "z"))
    wait("h2", "zc")
    xu1 = values_back("h2", pick1, block1)
    vals = vals + mm_t(xu1, oh0[:, 128:256])
    s1_all = total("u1_y", "y2")
    s1 = jnp.where(yb == 0, s1_all[0:8], s1_all[8:16]) * mc1
    g1 = (zp1 - mm_t(s1, cr1)) * mh1
    gs1 = jnp.concatenate([g1, -s1], axis=1)

    vals = vals + mm_t(gs1, ohq0)
    send["u0_zc"][...] = mm(jnp.where(front0, stack16(vals), 0.0), c0h).reshape(16, 8, 128)
    start("u0_zc", "zc")
    out[1] = zeta1 + mm_t(gs1, QW1)
    share("u0_x", "x", total("u0_zc", "zc"))
    s0 = total("u0_x", "x") * mc0
    g0 = (zp0 - mm_t(s0, cr0)) * mh0
    out[0] = zeta0 + mm_t(jnp.concatenate([g0, -s0], axis=1), QW0)

    for name, axis in pending:
        whole(name, axis).wait_send()


def apart(answers, *refs):
    copies = [pltpu.make_async_copy(answers.at[k], refs[k], refs[4].at[k]) for k in range(4)]
    for copy in copies:
        copy.start()
    for copy in copies:
        copy.wait()


def shards(*args):
    args = list(args)
    for i in (4, 12, 20, 28):
        args[i] = args[i].reshape(1, -1)
    for i in (7, 15, 23):
        args[i] = args[i].reshape(1, -1)
    for i in (6, 14):
        args[i] = args[i].T
    hbm = pl.BlockSpec(memory_space=pltpu.HBM)
    vmem = pl.BlockSpec(memory_space=pltpu.VMEM)
    sizes = {name: (n, rows, 128) for name, n, rows, _ in EXCHANGES}
    scratch = [pltpu.VMEM(arg.shape, arg.dtype) for arg in args]
    scratch += [pltpu.VMEM(sizes[name], jnp.float32) for name in NAMES]
    scratch += [pltpu.VMEM(sizes[name], jnp.float32) for name in SCATTERED]
    scratch += [pltpu.SemaphoreType.DMA((len(NAMES),)), pltpu.SemaphoreType.DMA((len(NAMES),))]
    scratch += [pltpu.SemaphoreType.DMA((len(args),))]
    answers = pl.pallas_call(
        kernel,
        out_shape=jax.ShapeDtypeStruct((4, 8, 128), jnp.float32),
        in_specs=[hbm] * len(args),
        out_specs=vmem,
        scratch_shapes=scratch,
        compiler_params=pltpu.CompilerParams(
            collective_id=0, has_side_effects=True, vmem_limit_bytes=67043328
        ),
        name="solve",
    )(*args)
    return tuple(
        pl.pallas_call(
            apart,
            out_shape=[jax.ShapeDtypeStruct((8, 128), jnp.float32)] * 4,
            in_specs=[hbm],
            out_specs=[hbm] * 4,
            scratch_shapes=[pltpu.SemaphoreType.DMA((4,))],
            name="apart",
        )(answers)
    )


def solution(mesh):
    columns = P(None, ("leaf", "grid"))
    rows = P(("leaf", "grid"), None)
    flat = P(("leaf", "grid"))
    level = (columns, rows, rows, rows, flat, rows, P(), flat)
    in_specs = level * 3 + (columns, rows, rows, rows, flat, P())
    return jax.shard_map(
        shards, mesh=mesh, in_specs=in_specs, out_specs=(columns,) * 4, check_vma=False
    )
```

```python
import functools

import jax
import jax.numpy as jnp
from jax import lax
from jax.experimental import pallas as pl
from jax.experimental.pallas import tpu as pltpu
from jax.sharding import PartitionSpec as P

MESH = pl.DeviceIdType.MESH
HIGH = lax.Precision.HIGH
HIGHEST = lax.Precision.HIGHEST

NX, NZC, NY = 4, 16, 4

EXCHANGES = [
    ("x0a", 4, 8, 8),
    ("x0b", 4, 8, 8),
    ("x0c", 4, 128, 128),
    ("zp0", 4, 8, 8),
    ("w0", 16, 8, 8),
    ("a1", 16, 24, 17),
    ("a2", 4, 72, 72),
    ("b1", 16, 16, 9),
    ("b2", 8, 24, 17),
    ("c1", 16, 24, 17),
    ("c2", 16, 24, 17),
    ("q_xc", 8, 16, 16),
    ("q_z", 8, 16, 16),
    ("q_g", 8, 16, 16),
    ("r_xc", 8, 32, 32),
    ("r_z", 8, 32, 32),
    ("r_y", 4, 32, 32),
    ("r_g", 8, 48, 48),
    ("f1_xc", 8, 16, 16),
    ("f1_z", 8, 16, 16),
    ("f1_y", 2, 8, 8),
    ("f2_c", 2, 8, 8),
    ("f2_k", 16, 8, 8),
    ("f2_z", 8, 16, 16),
    ("f2_g", 2, 16, 16),
    ("f3_c", 2, 8, 8),
    ("f3_k", 16, 8, 8),
    ("f3_z", 8, 8, 8),
    ("f3_g", 2, 8, 8),
    ("zp_xc", 8, 16, 16),
    ("zp_z", 8, 16, 16),
    ("zp_y", 2, 8, 8),
    ("d1", 16, 1, 1),
    ("d2", 8, 1, 1),
    ("e1", 16, 1, 1),
    ("e2", 16, 1, 1),
    ("u2_c", 2, 8, 8),
    ("u2_k", 16, 8, 8),
    ("u2_z", 8, 8, 8),
    ("u2_g", 2, 8, 8),
    ("g1", 16, 1, 1),
    ("g2", 16, 1, 1),
    ("u1_c", 2, 8, 8),
    ("u1_k", 8, 8, 8),
    ("u1_z", 8, 8, 8),
    ("u1_g", 2, 8, 8),
    ("h1", 8, 1, 1),
    ("h2", 16, 1, 1),
    ("u0_zc", 16, 8, 8),
    ("u0_x", 4, 8, 8),
]
NAMES = [entry[0] for entry in EXCHANGES]
SENT = {entry[0]: entry[3] for entry in EXCHANGES}
SCATTERED = [
    "a1", "a2", "b1", "b2", "c1", "c2", "q_xc", "r_xc", "d1", "d2", "e1", "e2", "f2_c", "f3_c", "u2_c", "u1_c", "g1", "g2", "h1", "h2", "u0_zc"
]


def dot(a, b, ca, cb, precision):
    return lax.dot_general(
        a, b, (((ca,), (cb,)), ((), ())), precision=precision, preferred_element_type=jnp.float32
    )


def mm(a, b, precision=HIGH):
    return dot(a, b, 1, 0, precision)


def mm_t(a, b, precision=HIGH):
    return dot(a, b, 1, 1, precision)


def t_mm(a, b, precision=HIGH):
    return dot(a, b, 0, 0, precision)


def iota(shape, dim):
    return lax.broadcasted_iota(jnp.int32, shape, dim)


def ones_where(cond):
    return jnp.where(cond, 1.0, 0.0).astype(jnp.float32)


def stack16(v):
    return jnp.concatenate([v] * 16, axis=0)


class Operand:
    def __init__(self, i, *refs):
        self.vmem = refs[31 + i]
        self.copy = pltpu.make_async_copy(refs[i], self.vmem, refs[-1].at[i])
        self.start = self.copy.start
        self.here = False

    def ready(self):
        if not self.here:
            self.copy.wait()
            self.here = True

    def __getitem__(self, index):
        self.ready()
        return self.vmem[index]

    def rank(self, side, front):
        if self.vmem.shape[1] == 2 and self.vmem.shape[0] < 3:
            column = self[:, side : side + 1].astype(jnp.float32)
            return jnp.sum(jnp.where(iota(column.shape, 0) == front, column, 0.0), axis=0, keepdims=True)
        row = self[side : side + 1, :].astype(jnp.float32)
        return jnp.sum(jnp.where(iota(row.shape, 1) == front, row, 0.0), axis=1, keepdims=True)


def kernel(*refs):
    (
        src0, blk0, exp0, bas0, piv0, cpl0, rnk0, tgt0,
        src1, blk1, exp1, bas1, piv1, cpl1, rnk1, tgt1,
        src2, blk2, exp2, bas2, piv2, cpl2, rnk2, tgt2,
        src3, blk3, exp3, bas3, piv3, rnk3,
        out,
    ) = [Operand(i, *refs) for i in range(30)] + list(refs[30:31])
    refs = refs[61:]
    n_ex = len(EXCHANGES)
    recv = dict(zip(NAMES, refs[:n_ex]))
    send = dict(zip(SCATTERED, refs[n_ex : n_ex + len(SCATTERED)]))
    send_sem, recv_sem = refs[n_ex + len(SCATTERED) : n_ex + len(SCATTERED) + 2]

    for operand in (tgt0, cpl0, src0, blk0, bas0, exp0):
        operand.start()

    leaf = lax.axis_index("leaf")
    x = lax.axis_index("grid")
    y = leaf // 16
    zc = leaf % 16
    z = zc // 2
    c = zc % 2
    u = y // 2
    yb = y % 2
    xc = x * 2 + c
    k8 = yb * 4 + x
    k16 = y * 4 + x

    axes = {
        "x": (x, 4, lambda d: (leaf, d)),
        "zc": (zc, 16, lambda d: (y * 16 + d, x)),
        "xc": (xc, 8, lambda d: (leaf - c + d % 2, d // 2)),
        "c": (c, 2, lambda d: (leaf - c + d, x)),
        "z": (z, 8, lambda d: (y * 16 + d * 2 + c, x)),
        "y2": (yb, 2, lambda d: ((u * 2 + d) * 16 + zc, x)),
        "y4": (y, 4, lambda d: (d * 16 + zc, x)),
        "k8": (k8, 8, lambda d: ((u * 2 + d // 4) * 16 + zc, d % 4)),
        "k16": (k16, 16, lambda d: ((d // 4) * 16 + zc, d % 4)),
    }
    pending = []

    def copy_of(name, src, dst, dev):
        i = NAMES.index(name)
        return pltpu.make_async_remote_copy(
            src_ref=src,
            dst_ref=dst,
            send_sem=send_sem.at[i],
            recv_sem=recv_sem.at[i],
            device_id=dev,
            device_id_type=MESH,
        )

    def start(name, axis):
        me, n, dev = axes[axis]
        buf = recv[name]
        scattered = name in send

        def body(o, carry):
            d = lax.rem(me + o, n)
            rows = pl.ds(0, SENT[name])
            src = send[name].at[d, rows] if scattered else buf.at[me, rows]
            copy_of(name, src, buf.at[me, rows], dev(d)).start()
            return carry

        if scattered:
            buf[me] = send[name][me]
        lax.fori_loop(1, n, body, 0)
        pending.append((name, axis))

    def whole(name, axis):
        me, n, dev = axes[axis]
        part = recv[name].at[pl.ds(0, n - 1), pl.ds(0, SENT[name])]
        return copy_of(name, part, part, dev(lax.rem(me + 1, n)))

    def wait(name, axis):
        whole(name, axis).wait_recv()

    def share(name, axis, value):
        recv[name][axes[axis][0]] = value
        start(name, axis)

    def total(name, axis):
        wait(name, axis)
        return jnp.sum(recv[name][...], axis=0)

    def scatter_halves(name, low, high):
        send[name][0] = low
        send[name][1] = high
        start(name, "c")

    barrier = pltpu.get_barrier_semaphore()

    def greet(axis):
        me, n, dev = axes[axis]

        def body(o, carry):
            pl.semaphore_signal(barrier, inc=1, device_id=dev(lax.rem(me + o, n)), device_id_type=MESH)
            return carry

        lax.fori_loop(1, n, body, 0)
        return n - 1

    greeted = greet("zc") + greet("k16") + greet("xc")

    for operand in (
        exp1, bas1, exp2, bas2, exp3, piv3, rnk0, piv0, tgt1, cpl1, tgt2, cpl2, src1, blk1, rnk1, piv1,
        src2, blk2, rnk2, piv2, src3, blk3, bas3, rnk3,
    ):
        operand.start()

    lane = iota((1, 128), 1)

    def mask_of(ref, front, side):
        return ones_where(lane.astype(jnp.float32) < ref.rank(side, front))

    def column(row):
        n = row.shape[1]
        return jnp.transpose(jnp.broadcast_to(row, (128, n)))

    def packets(targets, sep_bits, kbits, ranked):
        piece = targets >> sep_bits
        within = targets & ((1 << sep_bits) - 1)
        label = piece * 128 + (within & 127) + 1
        owner = within >> 7
        if ranked:
            n = targets.shape[1]
            of = owner.astype(jnp.float32)
            same = column(of)[:, 0:1] == of
            before = iota((n, n), 0) < iota((n, n), 1)
            order = jnp.sum(ones_where(same & before), axis=0, keepdims=True)
            return of * 4.0 + order, label.astype(jnp.float32)
        sub = owner & 63
        pos = ((sub >> 2) << kbits) + ((owner >> 6) << 2) + (sub & 3)
        return pos.astype(jnp.float32), label.astype(jnp.float32)

    def place(pos, count):
        n = pos.shape[1]
        return ones_where(iota((count, n), 0).astype(jnp.float32) == pos)

    def halves(pos, kbits):
        ipos = pos.astype(jnp.int32)
        return (ipos >> kbits).astype(jnp.float32), (ipos & ((1 << kbits) - 1)).astype(jnp.float32)

    def fill_packets(name, pos, label, kbits, couple):
        k = 1 << kbits
        n = pos.shape[1]
        send[name][:, 0:k, :] = mm(place(pos, 16 * k), couple, HIGHEST).reshape(16, k, 128)
        major, minor = halves(pos, kbits)
        pick = ones_where(iota((16, n), 0).astype(jnp.float32) == major)
        minor_col = column(minor)
        spread = jnp.where(iota((n, 128), 1).astype(jnp.float32) == minor_col, column(label), 0.0)
        labels = mm(pick, spread)
        send[name][:, k : k + 8, :] = jnp.broadcast_to(labels[:, None, :], (16, 8, 128))
        return pick, (iota((n, 128), 1) >> 3).astype(jnp.float32) == minor_col

    def chain(qv, w, p):
        return jnp.concatenate([qv, mm(w, p, HIGHEST)], axis=1)

    def label_rows(name, row, count, packet):
        labels = recv[name][:, row : row + 1, :].reshape(16, 128)
        labels = jnp.concatenate([labels, jnp.zeros((112, 128), jnp.float32)], axis=0)
        return mm_t(ones_where(iota((count, 128), 1) == packet(iota((count, 128), 0))), labels)

    def label_column(rows, bits):
        mine = iota(rows.shape, 1) == ((iota(rows.shape, 0) >> bits) & 15)
        return jnp.sum(jnp.where(mine, rows, 0.0), axis=1, keepdims=True)

    fold = ones_where((iota((128, 128), 0) & 7) == (iota((128, 128), 1) & 7))

    def blocks_are(shape_rows, of_row):
        return (iota((shape_rows, 128), 1) >> 3) == of_row(iota((shape_rows, 128), 0))

    def values_up(name, update, pick, block):
        rows = jnp.where(block, jnp.transpose(stack16(update)), 0.0)
        send[name][...] = mm(pick, rows).reshape(16, 1, 128)
        start(name, "zc")

    def values_on(name, got, outer, inner, axis):
        bits = inner.bit_length() - 1
        rows = jnp.concatenate([recv[got][...].reshape(inner, 128)] * outer, axis=0)
        rows = jnp.where(blocks_are(outer * inner, lambda r: r >> bits), rows, 0.0)
        rows = jnp.where(blocks_are(outer * inner, lambda r: r & (inner - 1)), mm(rows, fold), 0.0)
        send[name][...] = jnp.sum(rows.reshape(outer, inner, 128), axis=1).reshape(outer, 1, 128)
        start(name, axis)

    def values_in(got, k):
        rows = jnp.broadcast_to(recv[got][...], (k, 16, 128)).reshape(k * 16, 128)
        rows = jnp.where(blocks_are(k * 16, lambda r: r & 15), rows, 0.0)
        return mm_t(fold[0:8], rows)

    def values_down(name, onehot, full, k, axis):
        rows = mm_t(onehot, stack16(full))
        rows = jnp.where(blocks_are(k * 16, lambda r: r & 15), rows, 0.0)
        send[name][...] = jnp.sum(rows.reshape(k, 16, 128), axis=1).reshape(k, 1, 128)
        start(name, axis)

    def values_back(got, pick, block):
        rows = t_mm(pick, recv[got][...].reshape(16, 128))
        return mm_t(fold[0:8], jnp.where(block, rows, 0.0))

    pos0, lab0 = packets(tgt0[...], 13, 4, True)
    fill_packets("a1", pos0, lab0, 4, cpl0[...])
    Q0, V0 = bas0[:, 0:128], bas0[:, 128:256]
    t0 = mm(src0[...], Q0, HIGHEST)
    loc0 = mm(src0[...], blk0[...], HIGHEST)

    pl.semaphore_wait(barrier, greeted)
    share("x0a", "x", t0)
    start("a1", "zc")

    mh0, mc0 = mask_of(rnk0, leaf, 0), mask_of(rnk0, leaf, 1)
    V1 = bas1[:, 128:256]
    send["q_xc"][...] = t_mm(exp1[...], V1, HIGHEST).reshape(8, 16, 128)
    hq0 = total("x0a", "x") * mh0
    y0 = loc0 + mm_t(hq0, exp0[...], HIGHEST)
    share("x0b", "x", mm(y0, V0))
    start("q_xc", "xc")
    z0 = y0 * piv0[...]
    QW1 = chain(bas1[:, 0:128], blk1[...], V1)
    t1_src = mm(src1[...], QW1, HIGHEST)
    share("w0", "zc", total("x0b", "x") * mc0)
    share("zp0", "x", mm(z0, exp0[...], HIGHEST))

    s_row = iota((256, 256), 0)
    r_col = iota((256, 256), 1)
    turn_a = ones_where(r_col == ((s_row >> 2) & 15) * 16 + (s_row >> 6) * 4 + (s_row & 3))
    wait("a1", "zc")
    moved = mm(turn_a, recv["a1"][:, 0:16, :].reshape(256, 128), HIGHEST)
    send["a2"][:, 0:64, :] = moved.reshape(4, 64, 128)
    send["a2"][:, 64:72, :] = label_rows("a1", 16, 32, lambda r: (r >> 3) * 4 + (r & 3)).reshape(4, 8, 128)
    start("a2", "x")
    q_sum = total("q_xc", "xc")

    pos1, lab1 = packets(tgt1[...], 14, 3, False)
    pick1, block1 = fill_packets("b1", pos1, lab1, 3, cpl1[...])
    pos2, lab2 = packets(tgt2[...], 15, 4, False)
    pick2, block2 = fill_packets("c1", pos2, lab2, 4, cpl2[...])
    V2 = bas2[:, 128:256]
    P3 = exp3[...]
    send["r_xc"][:, 0:16, :] = t_mm(exp2[...], V2, HIGHEST).reshape(8, 16, 128)
    send["r_xc"][:, 16:32, :] = t_mm(P3, P3 * column(piv3[...]), HIGHEST).reshape(8, 16, 128)

    front0 = (iota((128, 256), 0) >> 3) == ((iota((128, 256), 1) & 63) >> 2)
    wait("w0", "zc")
    share("q_z", "z", q_sum)
    wait("a2", "x")
    c0h = recv["a2"][:, 0:64, :].reshape(256, 128)
    e0 = jnp.where(front0, mm_t(recv["w0"][...].reshape(128, 128), c0h), 0.0)
    slots = recv["a2"][:, 64:72, :]
    lab_col = label_column(jnp.concatenate([slots[v] for v in range(4) for _ in range(8)], axis=0), 2)
    oh0 = ones_where(iota((256, 256), 1).astype(jnp.float32) == lab_col - 1.0)
    inc0 = -mm(jnp.sum(e0.reshape(16, 8, 256), axis=0), oh0)
    t1 = t1_src + mm(inc0[:, 0:128], QW1)
    share("f1_xc", "xc", jnp.concatenate([t1[:, 0:128], t1[:, 128:256]], axis=0))
    values_up("d1", inc0[:, 128:256], pick1, block1)
    start("b1", "zc")
    loc1 = mm(src1[...] + inc0[:, 0:128], blk1[...], HIGHEST)
    ohq0 = mm(oh0[:, 0:128], QW1, HIGHEST)

    share("f1_z", "z", total("f1_xc", "xc"))
    share("q_g", "xc", total("q_z", "z"))
    start("r_xc", "xc")
    start("c1", "zc")
    QW2 = chain(bas2[:, 0:128], blk2[...], V2)
    t2_src = mm(src2[...], QW2, HIGHEST)
    wait("d1", "zc")
    values_on("d2", "d1", 8, 16, "k8")
    wait("b1", "zc")
    turn_b = ones_where(iota((128, 128), 1) == (iota((128, 128), 0) & 15) * 8 + (iota((128, 128), 0) >> 4))
    send["b2"][:, 0:16, :] = mm(turn_b, recv["b1"][:, 0:8, :].reshape(128, 128), HIGHEST).reshape(8, 16, 128)
    send["b2"][:, 16:17, :] = label_rows("b1", 8, 8, lambda r: r).reshape(8, 1, 128)
    start("b2", "k8")
    QW3 = chain(bas3[:, 0:128], blk3[...] * piv3[...], P3)
    t3_src = mm(src3[...], QW3, HIGHEST)
    turn_c = ones_where(r_col == (s_row & 15) * 16 + (s_row >> 4))

    mh1, mc1 = mask_of(rnk1, y, 0), mask_of(rnk1, y, 1)
    wait("q_g", "xc")
    cr1 = recv["q_g"][...].reshape(128, 128)
    tot1 = total("f1_z", "z")
    hq1 = tot1[0:8] * mh1
    share("f1_y", "y2", (tot1[8:16] + mm(hq1, cr1)) * mc1)
    share("r_z", "z", total("r_xc", "xc"))
    z1 = (loc1 + mm_t(hq1, exp1[...], HIGHEST)) * piv1[...]
    zp1_own = mm(z1, exp1[...], HIGHEST)
    zeta1 = mm_t(z1, blk1[...], HIGHEST)

    wait("b2", "k8")
    c1h = recv["b2"][:, 0:16, :].reshape(128, 128)
    lab_col = label_column(jnp.broadcast_to(recv["b2"][:, 16:17, :], (8, 16, 128)).reshape(128, 128), 0)
    oh1 = ones_where(iota((128, 256), 1).astype(jnp.float32) == lab_col - 1.0)
    ohq1 = mm(oh1[:, 0:128], QW2, HIGHEST)
    kl1 = jnp.concatenate([t_mm(c1h[0:64], ohq1[0:64], HIGHEST), t_mm(c1h[64:128], ohq1[64:128], HIGHEST)], axis=0)
    wait("d2", "k8")
    came1 = values_in("d2", 8)
    t2_src = t2_src + mm(came1, ohq1)
    inc1_came = mm(came1, oh1)
    wait("f1_y", "y2")
    w1 = recv["f1_y"]
    t2 = t2_src - mm(jnp.concatenate([w1[0], w1[1]], axis=1), kl1)
    scatter_halves("f2_c", t2[:, 0:128], t2[:, 128:256])
    front1 = (iota((16, 128), 0) >> 3) == (iota((16, 128), 1) >> 6)
    e1 = jnp.where(front1, mm_t(recv["f1_y"][...].reshape(16, 128), c1h), 0.0)
    inc1 = inc1_came - mm(e1[0:8] + e1[8:16], oh1)
    share("f2_k", "k16", total("f2_c", "c"))
    values_up("e1", inc1[:, 128:256], pick2, block2)
    share("r_y", "y4", total("r_z", "z"))
    loc2 = mm(src2[...] + inc1[:, 0:128], blk2[...], HIGHEST)
    wait("c1", "zc")
    send["c2"][:, 0:16, :] = mm(turn_c, recv["c1"][:, 0:16, :].reshape(256, 128), HIGHEST).reshape(16, 16, 128)
    send["c2"][:, 16:17, :] = label_rows("c1", 16, 16, lambda r: r).reshape(16, 1, 128)
    start("c2", "k16")
    wait("f2_k", "k16")
    fk = recv["f2_k"]
    share("f2_z", "z", jnp.concatenate([jnp.sum(fk[0:8], axis=0), jnp.sum(fk[8:16], axis=0)], axis=0))
    wait("e1", "zc")
    values_on("e2", "e1", 16, 16, "k16")
    wait("r_y", "y4")
    ry = recv["r_y"]
    share(
        "r_g",
        "xc",
        jnp.concatenate(
            [
                ry[0, 0:16, :] + ry[1, 0:16, :],
                ry[2, 0:16, :] + ry[3, 0:16, :],
                (ry[0, 16:32, :] + ry[1, 16:32, :]) + (ry[2, 16:32, :] + ry[3, 16:32, :]),
            ],
            axis=0,
        ),
    )
    wait("c2", "k16")
    c2h = recv["c2"][:, 0:16, :].reshape(256, 128)
    lab_col = label_column(jnp.broadcast_to(recv["c2"][:, 16:17, :], (16, 16, 128)).reshape(256, 128), 0)
    oh2 = ones_where(iota((256, 128), 1).astype(jnp.float32) == lab_col - 1.0)
    ohq2 = mm(oh2, QW3, HIGHEST)
    kl2 = jnp.concatenate([t_mm(c2h[0:128], ohq2[0:128], HIGHEST), t_mm(c2h[128:256], ohq2[128:256], HIGHEST)], axis=0)
    share("f2_g", "c", total("f2_z", "z"))
    wait("r_g", "xc")
    rg = recv["r_g"]
    cr2_each = [rg[:, 0:16, :].reshape(128, 128), rg[:, 16:32, :].reshape(128, 128)]
    m3 = rg[:, 32:48, :].reshape(128, 128)
    wait("e2", "k16")
    came2 = values_in("e2", 16)
    t3_src = t3_src + mm(came2, ohq2)
    wait("f2_g", "c")
    fg = recv["f2_g"]
    hq2_each, w2_each = [], []
    for v in range(2):
        t_q = fg[0, 8 * v : 8 * v + 8, :]
        t_v = fg[1, 8 * v : 8 * v + 8, :]
        hq = t_q * mask_of(rnk2, v, 0)
        hq2_each.append(hq)
        w2_each.append((t_v + mm(hq, cr2_each[v])) * mask_of(rnk2, v, 1))
    t3_w = mm(jnp.concatenate(w2_each, axis=1), kl2)
    front2 = (iota((16, 256), 0) >> 3) == (iota((16, 256), 1) >> 7)
    t3 = t3_src - t3_w
    scatter_halves("f3_c", t3[:, 0:128], t3[:, 128:256])
    first = u == 0
    hq2 = jnp.where(first, hq2_each[0], hq2_each[1])
    cr2 = jnp.where(first, cr2_each[0], cr2_each[1])
    mh2, mc2 = mask_of(rnk2, u, 0), mask_of(rnk2, u, 1)
    z2 = (loc2 + mm_t(hq2, exp2[...], HIGHEST)) * piv2[...]
    zp2_own = mm(z2, exp2[...], HIGHEST)
    share("f3_k", "k16", total("f3_c", "c"))
    e2 = jnp.where(front2, mm_t(jnp.concatenate(w2_each, axis=0), c2h), 0.0)
    b3 = src3[...] + mm(came2 - (e2[0:8] + e2[8:16]), oh2)
    loc3 = mm(b3, blk3[...])
    zeta3 = mm_t(loc3 * piv3[...], blk3[...])
    vals = mm_t(zeta3, oh2)
    u2_own = mm(jnp.where(front2, jnp.concatenate([vals, vals], axis=0), 0.0), c2h)
    share("f3_z", "z", total("f3_k", "k16"))
    share("zp_xc", "xc", jnp.concatenate([zp1_own, zp2_own], axis=0))
    zeta2 = mm_t(z2, blk2[...], HIGHEST)
    mh3 = mask_of(rnk3, 0, 0)
    QW0 = chain(Q0, blk0[...], V0)
    down1 = jnp.concatenate([t_mm(oh1[0:64], c1h[0:64]), t_mm(oh1[64:128], c1h[64:128])], axis=1)
    ks1, kx1 = down1[0:128], down1[128:256]
    share("f3_g", "c", total("f3_z", "z"))
    wait("f3_g", "c")
    hq3 = recv["f3_g"][0] * mh3
    g3 = (recv["f3_g"][1] + mm(hq3, m3)) * mh3
    gh3 = jnp.concatenate([g3, hq3], axis=1)

    u2_low = mm_t(gh3, kl2)
    scatter_halves("u2_c", u2_own[0:8] + u2_low[:, 0:128], u2_own[8:16] + u2_low[:, 128:256])
    x3 = zeta3 + mm_t(gh3, QW3)
    values_down("g1", oh2, x3, 16, "k16")
    share("u2_k", "k16", total("u2_c", "c"))
    share("zp_z", "z", total("zp_xc", "xc"))
    out[3] = x3
    u1_own = mm(zeta2, ks1)
    share("x0c", "x", t_mm(exp0[...], V0, HIGHEST))
    share("u2_z", "z", total("u2_k", "k16"))
    wait("g1", "k16")
    values_on("g2", "g1", 16, 16, "zc")
    zp_sum = total("zp_z", "z")
    zp1 = zp_sum[0:8]
    share("zp_y", "y2", zp_sum[8:16])
    share("u2_g", "c", total("u2_z", "z"))
    zp2 = total("zp_y", "y2")
    wait("g2", "zc")
    xu2 = values_back("g2", pick2, block2)
    u1_own = u1_own + mm(xu2, kx1)
    wait("u2_g", "c")
    s2 = recv["u2_g"][u] * mc2
    g2 = (zp2 - mm_t(s2, cr2)) * mh2
    gs2 = jnp.concatenate([g2, -s2], axis=1)

    u1_low = mm_t(gs2, kl1)
    scatter_halves("u1_c", u1_own[:, 0:128] + u1_low[:, 0:128], u1_own[:, 128:256] + u1_low[:, 128:256])
    x2 = zeta2 + mm_t(gs2, QW2)
    values_down("h1", oh1, jnp.concatenate([x2, xu2], axis=1), 8, "k8")
    share("u1_k", "k8", total("u1_c", "c"))
    out[2] = x2
    share("u1_z", "z", total("u1_k", "k8"))
    vals = mm_t(zeta1, oh0[:, 0:128])
    cr0 = total("x0c", "x")
    zp0 = total("zp0", "x")
    zeta0 = mm_t(z0, blk0[...], HIGHEST)
    wait("h1", "k8")
    values_on("h2", "h1", 16, 8, "zc")
    share("u1_g", "c", total("u1_z", "z"))
    wait("h2", "zc")
    xu1 = values_back("h2", pick1, block1)
    vals = vals + mm_t(xu1, oh0[:, 128:256])
    wait("u1_g", "c")
    s1 = recv["u1_g"][yb] * mc1
    g1 = (zp1 - mm_t(s1, cr1)) * mh1
    gs1 = jnp.concatenate([g1, -s1], axis=1)

    vals = vals + mm_t(gs1, ohq0)
    send["u0_zc"][...] = mm(jnp.where(front0, stack16(vals), 0.0), c0h).reshape(16, 8, 128)
    start("u0_zc", "zc")
    out[1] = zeta1 + mm_t(gs1, QW1, HIGHEST)
    share("u0_x", "x", total("u0_zc", "zc"))
    s0 = total("u0_x", "x") * mc0
    g0 = (zp0 - mm_t(s0, cr0)) * mh0
    out[0] = zeta0 + mm_t(jnp.concatenate([g0, -s0], axis=1), QW0)

    for name, axis in pending:
        whole(name, axis).wait_send()


def apart(answers, *refs):
    copies = [pltpu.make_async_copy(answers.at[k], refs[k], refs[4].at[k]) for k in range(4)]
    for copy in copies:
        copy.start()
    for copy in copies:
        copy.wait()


def shards(*args):
    args = list(args)
    for i in (4, 12, 20, 28):
        args[i] = args[i].reshape(1, -1)
    for i in (7, 15, 23):
        args[i] = args[i].reshape(1, -1)
    for i in (6, 14):
        args[i] = args[i].T
    hbm = pl.BlockSpec(memory_space=pltpu.HBM)
    vmem = pl.BlockSpec(memory_space=pltpu.VMEM)
    sizes = {name: (n, rows, 128) for name, n, rows, _ in EXCHANGES}
    scratch = [pltpu.VMEM(arg.shape, arg.dtype) for arg in args]
    scratch += [pltpu.VMEM(sizes[name], jnp.float32) for name in NAMES]
    scratch += [pltpu.VMEM(sizes[name], jnp.float32) for name in SCATTERED]
    scratch += [pltpu.SemaphoreType.DMA((len(NAMES),)), pltpu.SemaphoreType.DMA((len(NAMES),))]
    scratch += [pltpu.SemaphoreType.DMA((len(args),))]
    answers = pl.pallas_call(
        kernel,
        out_shape=jax.ShapeDtypeStruct((4, 8, 128), jnp.float32),
        in_specs=[hbm] * len(args),
        out_specs=vmem,
        scratch_shapes=scratch,
        compiler_params=pltpu.CompilerParams(
            collective_id=0, has_side_effects=True, vmem_limit_bytes=67043328
        ),
        name="solve",
    )(*args)
    return tuple(
        pl.pallas_call(
            apart,
            out_shape=[jax.ShapeDtypeStruct((8, 128), jnp.float32)] * 4,
            in_specs=[vmem],
            out_specs=[hbm] * 4,
            scratch_shapes=[pltpu.SemaphoreType.DMA((4,))],
            name="apart",
        )(answers)
    )


def solution(mesh):
    columns = P(None, ("leaf", "grid"))
    rows = P(("leaf", "grid"), None)
    flat = P(("leaf", "grid"))
    level = (columns, rows, rows, rows, flat, rows, P(), flat)
    in_specs = level * 3 + (columns, rows, rows, rows, flat, P())
    return jax.shard_map(
        shards, mesh=mesh, in_specs=in_specs, out_specs=(columns,) * 4, check_vma=False
    )
```

```python
import functools

import jax
import jax.numpy as jnp
from jax import lax
from jax.experimental import pallas as pl
from jax.experimental.pallas import tpu as pltpu
from jax.sharding import PartitionSpec as P

MESH = pl.DeviceIdType.MESH
HIGH = lax.Precision.HIGH
HIGHEST = lax.Precision.HIGHEST

NX, NZC, NY = 4, 16, 4

EXCHANGES = [
    ("x0a", 4, 8, 8),
    ("x0b", 4, 8, 8),
    ("x0c", 4, 128, 128),
    ("zp0", 4, 8, 8),
    ("w0", 16, 8, 8),
    ("a1", 16, 24, 17),
    ("a2", 4, 72, 72),
    ("b1", 16, 16, 9),
    ("b2", 8, 24, 17),
    ("c1", 16, 24, 17),
    ("c2", 16, 24, 17),
    ("q_xc", 8, 16, 16),
    ("q_z", 8, 16, 16),
    ("q_g", 8, 16, 16),
    ("r_xc", 8, 32, 32),
    ("r_z", 8, 32, 32),
    ("r_y", 4, 32, 32),
    ("r_g", 8, 48, 48),
    ("f1_xc", 8, 16, 16),
    ("f1_z", 8, 16, 16),
    ("f1_y", 2, 8, 8),
    ("f2_c", 2, 8, 8),
    ("f2_k", 16, 8, 8),
    ("f2_z", 8, 16, 16),
    ("f2_g", 2, 16, 16),
    ("f3_c", 2, 8, 8),
    ("f3_k", 16, 8, 8),
    ("f3_z", 8, 8, 8),
    ("f3_g", 2, 8, 8),
    ("zp_xc", 8, 16, 16),
    ("zp_z", 8, 16, 16),
    ("zp_y", 2, 8, 8),
    ("d1", 16, 1, 1),
    ("d2", 8, 1, 1),
    ("e1", 16, 1, 1),
    ("e2", 16, 1, 1),
    ("u2_c", 2, 8, 8),
    ("u2_k", 16, 8, 8),
    ("u2_z", 8, 8, 8),
    ("u2_g", 2, 8, 8),
    ("g1", 16, 1, 1),
    ("g2", 16, 1, 1),
    ("u1_c", 2, 8, 8),
    ("u1_k", 8, 8, 8),
    ("u1_z", 8, 8, 8),
    ("u1_g", 2, 8, 8),
    ("h1", 8, 1, 1),
    ("h2", 16, 1, 1),
    ("u0_zc", 16, 8, 8),
    ("u0_x", 4, 8, 8),
]
NAMES = [entry[0] for entry in EXCHANGES]
SENT = {entry[0]: entry[3] for entry in EXCHANGES}
SCATTERED = [
    "a1", "a2", "b1", "b2", "c1", "c2", "q_xc", "r_xc", "d1", "d2", "e1", "e2", "f2_c", "f3_c", "u2_c", "u1_c", "g1", "g2", "h1", "h2", "u0_zc"
]


def dot(a, b, ca, cb, precision):
    return lax.dot_general(
        a, b, (((ca,), (cb,)), ((), ())), precision=precision, preferred_element_type=jnp.float32
    )


def mm(a, b, precision=HIGH):
    return dot(a, b, 1, 0, precision)


def mm_t(a, b, precision=HIGH):
    return dot(a, b, 1, 1, precision)


def t_mm(a, b, precision=HIGH):
    return dot(a, b, 0, 0, precision)


def iota(shape, dim):
    return lax.broadcasted_iota(jnp.int32, shape, dim)


def ones_where(cond):
    return jnp.where(cond, 1.0, 0.0).astype(jnp.float32)


def stack16(v):
    return jnp.concatenate([v] * 16, axis=0)


class Operand:
    def __init__(self, i, *refs):
        self.vmem = refs[31 + i]
        self.copy = pltpu.make_async_copy(refs[i], self.vmem, refs[-1].at[i])
        self.start = self.copy.start
        self.here = False

    def ready(self):
        if not self.here:
            self.copy.wait()
            self.here = True

    def __getitem__(self, index):
        self.ready()
        return self.vmem[index]

    def rank(self, side, front):
        if self.vmem.shape[1] == 2 and self.vmem.shape[0] < 3:
            column = self[:, side : side + 1].astype(jnp.float32)
            return jnp.sum(jnp.where(iota(column.shape, 0) == front, column, 0.0), axis=0, keepdims=True)
        row = self[side : side + 1, :].astype(jnp.float32)
        return jnp.sum(jnp.where(iota(row.shape, 1) == front, row, 0.0), axis=1, keepdims=True)


def kernel(*refs):
    (
        src0, blk0, exp0, bas0, piv0, cpl0, rnk0, tgt0,
        src1, blk1, exp1, bas1, piv1, cpl1, rnk1, tgt1,
        src2, blk2, exp2, bas2, piv2, cpl2, rnk2, tgt2,
        src3, blk3, exp3, bas3, piv3, rnk3,
        out,
    ) = [Operand(i, *refs) for i in range(30)] + list(refs[30:31])
    refs = refs[61:]
    n_ex = len(EXCHANGES)
    recv = dict(zip(NAMES, refs[:n_ex]))
    send = dict(zip(SCATTERED, refs[n_ex : n_ex + len(SCATTERED)]))
    send_sem, recv_sem = refs[n_ex + len(SCATTERED) : n_ex + len(SCATTERED) + 2]

    for operand in (tgt0, cpl0, src0, blk0, bas0, exp0):
        operand.start()

    leaf = lax.axis_index("leaf")
    x = lax.axis_index("grid")
    y = leaf // 16
    zc = leaf % 16
    z = zc // 2
    c = zc % 2
    u = y // 2
    yb = y % 2
    xc = x * 2 + c
    k8 = yb * 4 + x
    k16 = y * 4 + x

    axes = {
        "x": (x, 4, lambda d: (leaf, d)),
        "zc": (zc, 16, lambda d: (y * 16 + d, x)),
        "xc": (xc, 8, lambda d: (leaf - c + d % 2, d // 2)),
        "c": (c, 2, lambda d: (leaf - c + d, x)),
        "z": (z, 8, lambda d: (y * 16 + d * 2 + c, x)),
        "y2": (yb, 2, lambda d: ((u * 2 + d) * 16 + zc, x)),
        "y4": (y, 4, lambda d: (d * 16 + zc, x)),
        "k8": (k8, 8, lambda d: ((u * 2 + d // 4) * 16 + zc, d % 4)),
        "k16": (k16, 16, lambda d: ((d // 4) * 16 + zc, d % 4)),
    }
    pending = []

    def copy_of(name, src, dst, dev):
        i = NAMES.index(name)
        return pltpu.make_async_remote_copy(
            src_ref=src,
            dst_ref=dst,
            send_sem=send_sem.at[i],
            recv_sem=recv_sem.at[i],
            device_id=dev,
            device_id_type=MESH,
        )

    def start(name, axis):
        me, n, dev = axes[axis]
        buf = recv[name]
        scattered = name in send

        def body(o, carry):
            d = lax.rem(me + o, n)
            rows = pl.ds(0, SENT[name])
            src = send[name].at[d, rows] if scattered else buf.at[me, rows]
            copy_of(name, src, buf.at[me, rows], dev(d)).start()
            return carry

        if scattered:
            buf[me] = send[name][me]
        lax.fori_loop(1, n, body, 0)
        pending.append((name, axis))

    def whole(name, axis):
        me, n, dev = axes[axis]
        part = recv[name].at[pl.ds(0, n - 1), pl.ds(0, SENT[name])]
        return copy_of(name, part, part, dev(lax.rem(me + 1, n)))

    def wait(name, axis):
        whole(name, axis).wait_recv()

    def share(name, axis, value):
        recv[name][axes[axis][0]] = value
        start(name, axis)

    def total(name, axis):
        wait(name, axis)
        return jnp.sum(recv[name][...], axis=0)

    def scatter_halves(name, low, high):
        send[name][0] = low
        send[name][1] = high
        start(name, "c")

    barrier = pltpu.get_barrier_semaphore()

    def greet(axis):
        me, n, dev = axes[axis]

        def body(o, carry):
            pl.semaphore_signal(barrier, inc=1, device_id=dev(lax.rem(me + o, n)), device_id_type=MESH)
            return carry

        lax.fori_loop(1, n, body, 0)
        return n - 1

    greeted = greet("zc") + greet("k16") + greet("xc")

    for operand in (
        exp1, bas1, exp2, bas2, exp3, piv3, rnk0, piv0, tgt1, cpl1, tgt2, cpl2, src1, blk1, rnk1, piv1,
        src2, blk2, rnk2, piv2, src3, blk3, bas3, rnk3,
    ):
        operand.start()

    lane = iota((1, 128), 1)

    def mask_of(ref, front, side):
        return ones_where(lane.astype(jnp.float32) < ref.rank(side, front))

    def column(row):
        n = row.shape[1]
        return jnp.transpose(jnp.broadcast_to(row, (128, n)))

    def packets(targets, sep_bits, kbits, ranked):
        piece = targets >> sep_bits
        within = targets & ((1 << sep_bits) - 1)
        label = piece * 128 + (within & 127) + 1
        owner = within >> 7
        if ranked:
            n = targets.shape[1]
            of = owner.astype(jnp.float32)
            same = column(of)[:, 0:1] == of
            before = iota((n, n), 0) < iota((n, n), 1)
            order = jnp.sum(ones_where(same & before), axis=0, keepdims=True)
            return of * 4.0 + order, label.astype(jnp.float32)
        sub = owner & 63
        pos = ((sub >> 2) << kbits) + ((owner >> 6) << 2) + (sub & 3)
        return pos.astype(jnp.float32), label.astype(jnp.float32)

    def place(pos, count):
        n = pos.shape[1]
        return ones_where(iota((count, n), 0).astype(jnp.float32) == pos)

    def halves(pos, kbits):
        ipos = pos.astype(jnp.int32)
        return (ipos >> kbits).astype(jnp.float32), (ipos & ((1 << kbits) - 1)).astype(jnp.float32)

    def fill_packets(name, pos, label, kbits, couple):
        k = 1 << kbits
        n = pos.shape[1]
        send[name][:, 0:k, :] = mm(place(pos, 16 * k), couple, HIGHEST).reshape(16, k, 128)
        major, minor = halves(pos, kbits)
        pick = ones_where(iota((16, n), 0).astype(jnp.float32) == major)
        minor_col = column(minor)
        spread = jnp.where(iota((n, 128), 1).astype(jnp.float32) == minor_col, column(label), 0.0)
        labels = mm(pick, spread)
        send[name][:, k : k + 8, :] = jnp.broadcast_to(labels[:, None, :], (16, 8, 128))
        return pick, (iota((n, 128), 1) >> 3).astype(jnp.float32) == minor_col

    def chain(qv, w, p):
        return jnp.concatenate([qv, mm(w, p, HIGHEST)], axis=1)

    def label_rows(name, row, count, packet):
        labels = recv[name][:, row : row + 1, :].reshape(16, 128)
        labels = jnp.concatenate([labels, jnp.zeros((112, 128), jnp.float32)], axis=0)
        return mm_t(ones_where(iota((count, 128), 1) == packet(iota((count, 128), 0))), labels)

    def label_column(rows, bits):
        mine = iota(rows.shape, 1) == ((iota(rows.shape, 0) >> bits) & 15)
        return jnp.sum(jnp.where(mine, rows, 0.0), axis=1, keepdims=True)

    fold = ones_where((iota((128, 128), 0) & 7) == (iota((128, 128), 1) & 7))

    def blocks_are(shape_rows, of_row):
        return (iota((shape_rows, 128), 1) >> 3) == of_row(iota((shape_rows, 128), 0))

    def values_up(name, update, pick, block):
        rows = jnp.where(block, jnp.transpose(stack16(update)), 0.0)
        send[name][...] = mm(pick, rows).reshape(16, 1, 128)
        start(name, "zc")

    def values_on(name, got, outer, inner, axis):
        bits = inner.bit_length() - 1
        rows = jnp.concatenate([recv[got][...].reshape(inner, 128)] * outer, axis=0)
        rows = jnp.where(blocks_are(outer * inner, lambda r: r >> bits), rows, 0.0)
        rows = jnp.where(blocks_are(outer * inner, lambda r: r & (inner - 1)), mm(rows, fold), 0.0)
        send[name][...] = jnp.sum(rows.reshape(outer, inner, 128), axis=1).reshape(outer, 1, 128)
        start(name, axis)

    def values_in(got, k):
        rows = jnp.broadcast_to(recv[got][...], (k, 16, 128)).reshape(k * 16, 128)
        rows = jnp.where(blocks_are(k * 16, lambda r: r & 15), rows, 0.0)
        return mm_t(fold[0:8], rows)

    def values_down(name, onehot, full, k, axis):
        rows = mm_t(onehot, stack16(full))
        rows = jnp.where(blocks_are(k * 16, lambda r: r & 15), rows, 0.0)
        send[name][...] = jnp.sum(rows.reshape(k, 16, 128), axis=1).reshape(k, 1, 128)
        start(name, axis)

    def values_back(got, pick, block):
        rows = t_mm(pick, recv[got][...].reshape(16, 128))
        return mm_t(fold[0:8], jnp.where(block, rows, 0.0))

    pos0, lab0 = packets(tgt0[...], 13, 4, True)
    fill_packets("a1", pos0, lab0, 4, cpl0[...])
    Q0, V0 = bas0[:, 0:128], bas0[:, 128:256]
    t0 = mm(src0[...], Q0, HIGHEST)
    loc0 = mm(src0[...], blk0[...], HIGHEST)

    cr0_own = t_mm(exp0[...], V0, HIGHEST)
    w0_own = mm(loc0, V0, HIGHEST)

    pl.semaphore_wait(barrier, greeted)
    share("x0a", "x", t0)
    start("a1", "zc")

    mh0, mc0 = mask_of(rnk0, leaf, 0), mask_of(rnk0, leaf, 1)
    V1 = bas1[:, 128:256]
    send["q_xc"][...] = t_mm(exp1[...], V1, HIGHEST).reshape(8, 16, 128)
    hq0 = total("x0a", "x") * mh0
    share("x0b", "x", w0_own + mm(hq0, cr0_own))
    start("q_xc", "xc")
    z0 = (loc0 + mm_t(hq0, exp0[...], HIGHEST)) * piv0[...]
    QW1 = chain(bas1[:, 0:128], blk1[...], V1)
    t1_src = mm(src1[...], QW1, HIGHEST)
    share("w0", "zc", total("x0b", "x") * mc0)
    share("zp0", "x", mm(z0, exp0[...], HIGHEST))

    s_row = iota((256, 256), 0)
    r_col = iota((256, 256), 1)
    turn_a = ones_where(r_col == ((s_row >> 2) & 15) * 16 + (s_row >> 6) * 4 + (s_row & 3))
    wait("a1", "zc")
    moved = mm(turn_a, recv["a1"][:, 0:16, :].reshape(256, 128), HIGHEST)
    send["a2"][:, 0:64, :] = moved.reshape(4, 64, 128)
    send["a2"][:, 64:72, :] = label_rows("a1", 16, 32, lambda r: (r >> 3) * 4 + (r & 3)).reshape(4, 8, 128)
    start("a2", "x")
    q_sum = total("q_xc", "xc")

    pos1, lab1 = packets(tgt1[...], 14, 3, False)
    pick1, block1 = fill_packets("b1", pos1, lab1, 3, cpl1[...])
    pos2, lab2 = packets(tgt2[...], 15, 4, False)
    pick2, block2 = fill_packets("c1", pos2, lab2, 4, cpl2[...])
    V2 = bas2[:, 128:256]
    P3 = exp3[...]
    send["r_xc"][:, 0:16, :] = t_mm(exp2[...], V2, HIGHEST).reshape(8, 16, 128)
    send["r_xc"][:, 16:32, :] = t_mm(P3, P3 * column(piv3[...]), HIGHEST).reshape(8, 16, 128)

    front0 = (iota((128, 256), 0) >> 3) == ((iota((128, 256), 1) & 63) >> 2)
    wait("w0", "zc")
    share("q_z", "z", q_sum)
    wait("a2", "x")
    c0h = recv["a2"][:, 0:64, :].reshape(256, 128)
    e0 = jnp.where(front0, mm_t(recv["w0"][...].reshape(128, 128), c0h), 0.0)
    slots = recv["a2"][:, 64:72, :]
    lab_col = label_column(jnp.concatenate([slots[v] for v in range(4) for _ in range(8)], axis=0), 2)
    oh0 = ones_where(iota((256, 256), 1).astype(jnp.float32) == lab_col - 1.0)
    inc0 = -mm(jnp.sum(e0.reshape(16, 8, 256), axis=0), oh0)
    t1 = t1_src + mm(inc0[:, 0:128], QW1)
    share("f1_xc", "xc", jnp.concatenate([t1[:, 0:128], t1[:, 128:256]], axis=0))
    values_up("d1", inc0[:, 128:256], pick1, block1)
    start("b1", "zc")
    loc1 = mm(src1[...] + inc0[:, 0:128], blk1[...], HIGHEST)
    ohq0 = mm(oh0[:, 0:128], QW1, HIGHEST)

    share("f1_z", "z", total("f1_xc", "xc"))
    share("q_g", "xc", total("q_z", "z"))
    start("r_xc", "xc")
    start("c1", "zc")
    QW2 = chain(bas2[:, 0:128], blk2[...], V2)
    t2_src = mm(src2[...], QW2, HIGHEST)
    wait("d1", "zc")
    values_on("d2", "d1", 8, 16, "k8")
    wait("b1", "zc")
    turn_b = ones_where(iota((128, 128), 1) == (iota((128, 128), 0) & 15) * 8 + (iota((128, 128), 0) >> 4))
    send["b2"][:, 0:16, :] = mm(turn_b, recv["b1"][:, 0:8, :].reshape(128, 128), HIGHEST).reshape(8, 16, 128)
    send["b2"][:, 16:17, :] = label_rows("b1", 8, 8, lambda r: r).reshape(8, 1, 128)
    start("b2", "k8")
    QW3 = chain(bas3[:, 0:128], blk3[...] * piv3[...], P3)
    t3_src = mm(src3[...], QW3, HIGHEST)
    turn_c = ones_where(r_col == (s_row & 15) * 16 + (s_row >> 4))

    mh1, mc1 = mask_of(rnk1, y, 0), mask_of(rnk1, y, 1)
    wait("q_g", "xc")
    cr1 = recv["q_g"][...].reshape(128, 128)
    tot1 = total("f1_z", "z")
    hq1 = tot1[0:8] * mh1
    share("f1_y", "y2", (tot1[8:16] + mm(hq1, cr1)) * mc1)
    share("r_z", "z", total("r_xc", "xc"))
    z1 = (loc1 + mm_t(hq1, exp1[...], HIGHEST)) * piv1[...]
    zp1_own = mm(z1, exp1[...], HIGHEST)
    zeta1 = mm_t(z1, blk1[...], HIGHEST)

    wait("b2", "k8")
    c1h = recv["b2"][:, 0:16, :].reshape(128, 128)
    lab_col = label_column(jnp.broadcast_to(recv["b2"][:, 16:17, :], (8, 16, 128)).reshape(128, 128), 0)
    oh1 = ones_where(iota((128, 256), 1).astype(jnp.float32) == lab_col - 1.0)
    ohq1 = mm(oh1[:, 0:128], QW2, HIGHEST)
    kl1 = jnp.concatenate([t_mm(c1h[0:64], ohq1[0:64], HIGHEST), t_mm(c1h[64:128], ohq1[64:128], HIGHEST)], axis=0)
    wait("d2", "k8")
    came1 = values_in("d2", 8)
    t2_src = t2_src + mm(came1, ohq1)
    inc1_came = mm(came1, oh1)
    wait("f1_y", "y2")
    w1 = recv["f1_y"]
    t2 = t2_src - mm(jnp.concatenate([w1[0], w1[1]], axis=1), kl1)
    scatter_halves("f2_c", t2[:, 0:128], t2[:, 128:256])
    front1 = (iota((16, 128), 0) >> 3) == (iota((16, 128), 1) >> 6)
    e1 = jnp.where(front1, mm_t(recv["f1_y"][...].reshape(16, 128), c1h), 0.0)
    inc1 = inc1_came - mm(e1[0:8] + e1[8:16], oh1)
    share("f2_k", "k16", total("f2_c", "c"))
    values_up("e1", inc1[:, 128:256], pick2, block2)
    share("r_y", "y4", total("r_z", "z"))
    loc2 = mm(src2[...] + inc1[:, 0:128], blk2[...], HIGHEST)
    wait("c1", "zc")
    send["c2"][:, 0:16, :] = mm(turn_c, recv["c1"][:, 0:16, :].reshape(256, 128), HIGHEST).reshape(16, 16, 128)
    send["c2"][:, 16:17, :] = label_rows("c1", 16, 16, lambda r: r).reshape(16, 1, 128)
    start("c2", "k16")
    wait("f2_k", "k16")
    fk = recv["f2_k"]
    share("f2_z", "z", jnp.concatenate([jnp.sum(fk[0:8], axis=0), jnp.sum(fk[8:16], axis=0)], axis=0))
    wait("e1", "zc")
    values_on("e2", "e1", 16, 16, "k16")
    wait("r_y", "y4")
    ry = recv["r_y"]
    share(
        "r_g",
        "xc",
        jnp.concatenate(
            [
                ry[0, 0:16, :] + ry[1, 0:16, :],
                ry[2, 0:16, :] + ry[3, 0:16, :],
                (ry[0, 16:32, :] + ry[1, 16:32, :]) + (ry[2, 16:32, :] + ry[3, 16:32, :]),
            ],
            axis=0,
        ),
    )
    wait("c2", "k16")
    c2h = recv["c2"][:, 0:16, :].reshape(256, 128)
    lab_col = label_column(jnp.broadcast_to(recv["c2"][:, 16:17, :], (16, 16, 128)).reshape(256, 128), 0)
    oh2 = ones_where(iota((256, 128), 1).astype(jnp.float32) == lab_col - 1.0)
    ohq2 = mm(oh2, QW3, HIGHEST)
    kl2 = jnp.concatenate([t_mm(c2h[0:128], ohq2[0:128], HIGHEST), t_mm(c2h[128:256], ohq2[128:256], HIGHEST)], axis=0)
    share("f2_g", "c", total("f2_z", "z"))
    wait("r_g", "xc")
    rg = recv["r_g"]
    cr2_each = [rg[:, 0:16, :].reshape(128, 128), rg[:, 16:32, :].reshape(128, 128)]
    m3 = rg[:, 32:48, :].reshape(128, 128)
    wait("e2", "k16")
    came2 = values_in("e2", 16)
    t3_src = t3_src + mm(came2, ohq2)
    wait("f2_g", "c")
    fg = recv["f2_g"]
    hq2_each, w2_each = [], []
    for v in range(2):
        t_q = fg[0, 8 * v : 8 * v + 8, :]
        t_v = fg[1, 8 * v : 8 * v + 8, :]
        hq = t_q * mask_of(rnk2, v, 0)
        hq2_each.append(hq)
        w2_each.append((t_v + mm(hq, cr2_each[v])) * mask_of(rnk2, v, 1))
    t3_w = mm(jnp.concatenate(w2_each, axis=1), kl2)
    front2 = (iota((16, 256), 0) >> 3) == (iota((16, 256), 1) >> 7)
    t3 = t3_src - t3_w
    scatter_halves("f3_c", t3[:, 0:128], t3[:, 128:256])
    first = u == 0
    hq2 = jnp.where(first, hq2_each[0], hq2_each[1])
    cr2 = jnp.where(first, cr2_each[0], cr2_each[1])
    mh2, mc2 = mask_of(rnk2, u, 0), mask_of(rnk2, u, 1)
    z2 = (loc2 + mm_t(hq2, exp2[...], HIGHEST)) * piv2[...]
    zp2_own = mm(z2, exp2[...], HIGHEST)
    share("f3_k", "k16", total("f3_c", "c"))
    e2 = jnp.where(front2, mm_t(jnp.concatenate(w2_each, axis=0), c2h), 0.0)
    b3 = src3[...] + mm(came2 - (e2[0:8] + e2[8:16]), oh2)
    loc3 = mm(b3, blk3[...])
    zeta3 = mm_t(loc3 * piv3[...], blk3[...])
    vals = mm_t(zeta3, oh2)
    u2_own = mm(jnp.where(front2, jnp.concatenate([vals, vals], axis=0), 0.0), c2h)
    share("f3_z", "z", total("f3_k", "k16"))
    share("zp_xc", "xc", jnp.concatenate([zp1_own, zp2_own], axis=0))
    zeta2 = mm_t(z2, blk2[...], HIGHEST)
    mh3 = mask_of(rnk3, 0, 0)
    QW0 = chain(Q0, blk0[...], V0)
    m3 = m3 * mh3
    low2 = jnp.concatenate([kl2[:, 128:256] + mm_t(kl2[:, 0:128], m3, HIGHEST), kl2[:, 0:128]], axis=1)
    low1 = kl1[:, 128:256] + mm(kl1[:, 0:128] * mh2, cr2, HIGHEST)
    QR2 = QW2[:, 128:256] + mm(QW2[:, 0:128] * mh2, cr2, HIGHEST)
    down1 = jnp.concatenate([t_mm(oh1[0:64], c1h[0:64]), t_mm(oh1[64:128], c1h[64:128])], axis=1)
    ks1, kx1 = down1[0:128], down1[128:256]
    share("f3_g", "c", total("f3_z", "z"))
    wait("f3_g", "c")
    hq3 = recv["f3_g"][0] * mh3
    half3 = recv["f3_g"][1] * mh3

    u2_low = mm_t(jnp.concatenate([hq3, half3], axis=1), low2)
    scatter_halves("u2_c", u2_own[0:8] + u2_low[:, 0:128], u2_own[8:16] + u2_low[:, 128:256])
    x3 = zeta3 + mm_t(jnp.concatenate([half3 + mm(hq3, m3), hq3], axis=1), QW3)
    values_down("g1", oh2, x3, 16, "k16")
    share("u2_k", "k16", total("u2_c", "c"))
    share("zp_z", "z", total("zp_xc", "xc"))
    out[3] = x3
    u1_own = mm(zeta2, ks1)
    share("x0c", "x", cr0_own)
    share("u2_z", "z", total("u2_k", "k16"))
    wait("g1", "k16")
    values_on("g2", "g1", 16, 16, "zc")
    zp_sum = total("zp_z", "z")
    zp1 = zp_sum[0:8]
    share("zp_y", "y2", zp_sum[8:16])
    share("u2_g", "c", total("u2_z", "z"))
    zp2 = total("zp_y", "y2") * mh2
    u1_own = u1_own + mm_t(zp2, kl1[:, 0:128])
    x2_own = zeta2 + mm_t(zp2, QW2[:, 0:128])
    low0 = ohq0[:, 128:256] + mm(ohq0[:, 0:128] * mh1, cr1, HIGHEST)
    QR1 = QW1[:, 128:256] + mm(QW1[:, 0:128] * mh1, cr1, HIGHEST)
    wait("g2", "zc")
    xu2 = values_back("g2", pick2, block2)
    u1_own = u1_own + mm(xu2, kx1)
    wait("u2_g", "c")
    s2 = recv["u2_g"][u] * mc2

    u1_own = u1_own - mm_t(s2, low1)
    scatter_halves("u1_c", u1_own[:, 0:128], u1_own[:, 128:256])
    x2 = x2_own - mm_t(s2, QR2)
    values_down("h1", oh1, jnp.concatenate([x2, xu2], axis=1), 8, "k8")
    share("u1_k", "k8", total("u1_c", "c"))
    out[2] = x2
    share("u1_z", "z", total("u1_k", "k8"))
    zp1 = zp1 * mh1
    vals = mm_t(zeta1, oh0[:, 0:128]) + mm_t(zp1, ohq0[:, 0:128])
    x1_own = zeta1 + mm_t(zp1, QW1[:, 0:128])
    cr0 = total("x0c", "x")
    zp0 = total("zp0", "x")
    zeta0 = mm_t(z0, blk0[...], HIGHEST)
    wait("h1", "k8")
    values_on("h2", "h1", 16, 8, "zc")
    share("u1_g", "c", total("u1_z", "z"))
    wait("h2", "zc")
    xu1 = values_back("h2", pick1, block1)
    vals = vals + mm_t(xu1, oh0[:, 128:256])
    wait("u1_g", "c")
    s1 = recv["u1_g"][yb] * mc1

    vals = vals - mm_t(s1, low0)
    send["u0_zc"][...] = mm(jnp.where(front0, stack16(vals), 0.0), c0h).reshape(16, 8, 128)
    start("u0_zc", "zc")
    out[1] = x1_own - mm_t(s1, QR1, HIGHEST)
    zp0 = zp0 * mh0
    x0_own = zeta0 + mm_t(zp0, Q0, HIGHEST)
    QR0 = QW0[:, 128:256] + mm(Q0 * mh0, cr0, HIGHEST)
    share("u0_x", "x", total("u0_zc", "zc"))
    s0 = total("u0_x", "x") * mc0
    out[0] = x0_own - mm_t(s0, QR0)

    for name, axis in pending:
        whole(name, axis).wait_send()


def apart(answers, *refs):
    copies = [pltpu.make_async_copy(answers.at[k], refs[k], refs[4].at[k]) for k in range(4)]
    for copy in copies:
        copy.start()
    for copy in copies:
        copy.wait()


def shards(*args):
    args = list(args)
    for i in (4, 12, 20, 28):
        args[i] = args[i].reshape(1, -1)
    for i in (7, 15, 23):
        args[i] = args[i].reshape(1, -1)
    for i in (6, 14):
        args[i] = args[i].T
    hbm = pl.BlockSpec(memory_space=pltpu.HBM)
    vmem = pl.BlockSpec(memory_space=pltpu.VMEM)
    sizes = {name: (n, rows, 128) for name, n, rows, _ in EXCHANGES}
    scratch = [pltpu.VMEM(arg.shape, arg.dtype) for arg in args]
    scratch += [pltpu.VMEM(sizes[name], jnp.float32) for name in NAMES]
    scratch += [pltpu.VMEM(sizes[name], jnp.float32) for name in SCATTERED]
    scratch += [pltpu.SemaphoreType.DMA((len(NAMES),)), pltpu.SemaphoreType.DMA((len(NAMES),))]
    scratch += [pltpu.SemaphoreType.DMA((len(args),))]
    answers = pl.pallas_call(
        kernel,
        out_shape=jax.ShapeDtypeStruct((4, 8, 128), jnp.float32),
        in_specs=[hbm] * len(args),
        out_specs=vmem,
        scratch_shapes=scratch,
        compiler_params=pltpu.CompilerParams(
            collective_id=0, has_side_effects=True, vmem_limit_bytes=48 * 1024 * 1024
        ),
        name="solve",
    )(*[pltpu.with_memory_space_constraint(a, pltpu.HBM) for a in args])
    return tuple(
        pl.pallas_call(
            apart,
            out_shape=[jax.ShapeDtypeStruct((8, 128), jnp.float32)] * 4,
            in_specs=[vmem],
            out_specs=[hbm] * 4,
            scratch_shapes=[pltpu.SemaphoreType.DMA((4,))],
            compiler_params=pltpu.CompilerParams(vmem_limit_bytes=1024 * 1024),
            name="apart",
        )(answers)
    )


def solution(mesh):
    columns = P(None, ("leaf", "grid"))
    rows = P(("leaf", "grid"), None)
    flat = P(("leaf", "grid"))
    level = (columns, rows, rows, rows, flat, rows, P(), flat)
    in_specs = level * 3 + (columns, rows, rows, rows, flat, P())
    return jax.shard_map(
        shards, mesh=mesh, in_specs=in_specs, out_specs=(columns,) * 4, check_vma=False
    )
```
